32 devices in a mesh: dp: 4 (over z), sh: 8 (over y, x, core).
Axes of the slice: x: 2, y: 2, z: 4, core: 2. Of those that a mesh axis runs over, the one named last changes fastest.
Arguments:
- k_prefill: bfloat16 [32, 4352, 8, 128], P('dp', None, 'sh'), parts along dimension 0
- v_prefill: bfloat16 [32, 4352, 8, 128], P('dp', None, 'sh'), parts along dimension 0
- lengths: int32 [32], P('dp'), parts along dimension 0
- residual: bfloat16 [32, 4096], P(('dp', 'sh')), parts along dimension 0
- norm_gain: bfloat16 [4096], replicated
- w_query: bfloat16 [4096, 4096], replicated
- w_key: bfloat16 [4096, 1024], replicated
- w_value: bfloat16 [4096, 1024], replicated
- w_out: bfloat16 [4096, 4096], replicated
Outputs:
- output 1: bfloat16 [32, 4096], P(('dp', 'sh')), parts along dimension 0
- output 2: bfloat16 [32, 4096, 8, 128], P(('dp', 'sh')), parts along dimension 0
- output 3: bfloat16 [32, 4096, 8, 128], P(('dp', 'sh')), parts along dimension 0
There are 4 independent parts. The reference program is written for one: setup_inputs(seed, part) draws one part's arguments, and reference() takes and returns one part's arrays. A program takes and returns all parts, laid end to end along the dimension named above; an argument that names none is the same for every part.
All inputs are finite; a program needn't handle non-finite values.
Results may differ from the reference program's by a relative error of at most 0.00421.
Values are sent between devices in bfloat16 or wider.
A program may use at most 1 GiB of HBM per device.

```python
import jax
import jax.numpy as jnp
from jax import lax

MODEL_DIM = 4096
HEADS = 32
KV_HEADS = 8
HEAD_DIM = 128
WINDOW = 4096
SEQ_LEN = 4352
BATCH = 8
Q_GROUP = HEADS // KV_HEADS
Q_WIDTH = HEADS * HEAD_DIM
KV_WIDTH = KV_HEADS * HEAD_DIM
THETA = 10000.0
EPS = 1e-5


def setup_inputs(seed: int = 0, part: int = 0) -> dict:
    root_key = jax.random.key(seed)
    part_root, shared_root = jax.random.split(root_key)
    part_keys = jax.random.split(jax.random.fold_in(part_root, part), 4)
    shared_keys = jax.random.split(shared_root, 5)
    kv_shape = (BATCH, SEQ_LEN, KV_HEADS, HEAD_DIM)
    k_prefill = jax.random.normal(part_keys[0], kv_shape, jnp.float32).astype(jnp.bfloat16)
    v_prefill = jax.random.normal(part_keys[1], kv_shape, jnp.float32).astype(jnp.bfloat16)
    lengths = jax.random.randint(part_keys[2], (BATCH,), 1, SEQ_LEN + 1, dtype=jnp.int32)
    lengths = lengths.at[0].set(SEQ_LEN).at[1].set(1)
    residual = jax.random.normal(part_keys[3], (BATCH, MODEL_DIM), jnp.float32).astype(jnp.bfloat16)
    norm_gain = (1.0 + 0.3 * jax.random.normal(shared_keys[0], (MODEL_DIM,), jnp.float32)).astype(jnp.bfloat16)
    w_query = (jax.random.normal(shared_keys[1], (MODEL_DIM, Q_WIDTH), jnp.float32) * (2.0 / MODEL_DIM ** 0.5)).astype(jnp.bfloat16)
    w_key = (jax.random.normal(shared_keys[2], (MODEL_DIM, KV_WIDTH), jnp.float32) * (3.0 / MODEL_DIM ** 0.5)).astype(jnp.bfloat16)
    w_value = (jax.random.normal(shared_keys[3], (MODEL_DIM, KV_WIDTH), jnp.float32) * (3.0 / MODEL_DIM ** 0.5)).astype(jnp.bfloat16)
    w_out = (jax.random.normal(shared_keys[4], (Q_WIDTH, MODEL_DIM), jnp.float32) * (2.0 / Q_WIDTH ** 0.5)).astype(jnp.bfloat16)
    return {'k_prefill': k_prefill, 'v_prefill': v_prefill, 'lengths': lengths, 'residual': residual, 'norm_gain': norm_gain, 'w_query': w_query, 'w_key': w_key, 'w_value': w_value, 'w_out': w_out}


def rolling_cache(prefill, lengths):
    slot_ids = jnp.arange(WINDOW, dtype=jnp.int32)
    last_pos = lengths[:, None] - 1
    held_pos = last_pos - jnp.remainder(last_pos - slot_ids[None, :], WINDOW)
    held = jax.vmap(lambda row_vals, row_idx: jnp.take(row_vals, row_idx, axis=0))(prefill, jnp.maximum(held_pos, 0))
    return jnp.where((held_pos >= 0)[:, :, None, None], held, jnp.zeros((), prefill.dtype))


def rotate(heads, positions):
    half_dim = HEAD_DIM // 2
    inv_freq = THETA ** (-2.0 * jnp.arange(half_dim, dtype=jnp.float32) / HEAD_DIM)
    angles = positions.astype(jnp.float32).reshape(positions.shape + (1,) * (heads.ndim - 1)) * inv_freq
    cos_part = jnp.cos(angles)
    sin_part = jnp.sin(angles)
    first_half = heads[..., :half_dim].astype(jnp.float32)
    second_half = heads[..., half_dim:].astype(jnp.float32)
    return jnp.concatenate([first_half * cos_part - second_half * sin_part, second_half * cos_part + first_half * sin_part], axis=-1).astype(jnp.bfloat16)


def attend_row(row_args):
    q_row, k_row, v_row, live_row = row_args
    q_grouped = q_row.reshape(KV_HEADS, Q_GROUP, HEAD_DIM).astype(jnp.float32)
    scores = jnp.einsum('kgd,wkd->kgw', q_grouped, k_row.astype(jnp.float32)) / HEAD_DIM ** 0.5
    scores = jnp.where(live_row[None, None, :], scores, -jnp.inf)
    weights = jax.nn.softmax(scores, axis=-1).astype(jnp.bfloat16)
    mixed = jnp.einsum('kgw,wkd->kgd', weights.astype(jnp.float32), v_row.astype(jnp.float32))
    return mixed.astype(jnp.bfloat16).reshape(Q_WIDTH)


def reference(k_prefill, v_prefill, lengths, residual, norm_gain, w_query, w_key, w_value, w_out):
    k_cache = rolling_cache(k_prefill, lengths)
    v_cache = rolling_cache(v_prefill, lengths)
    resid_f32 = residual.astype(jnp.float32)
    inv_rms = lax.rsqrt(jnp.mean(resid_f32 * resid_f32, axis=-1, keepdims=True) + EPS)
    normed = (resid_f32 * inv_rms * norm_gain.astype(jnp.float32)).astype(jnp.bfloat16)
    q_heads = jnp.dot(normed, w_query, preferred_element_type=jnp.float32).astype(jnp.bfloat16).reshape(BATCH, HEADS, HEAD_DIM)
    k_new = jnp.dot(normed, w_key, preferred_element_type=jnp.float32).astype(jnp.bfloat16).reshape(BATCH, KV_HEADS, HEAD_DIM)
    v_new = jnp.dot(normed, w_value, preferred_element_type=jnp.float32).astype(jnp.bfloat16).reshape(BATCH, KV_HEADS, HEAD_DIM)
    q_heads = rotate(q_heads, lengths)
    k_new = rotate(k_new, lengths)
    slot_ids = jnp.arange(WINDOW, dtype=jnp.int32)
    new_slot = (slot_ids[None, :] == (lengths % WINDOW)[:, None])[:, :, None, None]
    k_cache = jnp.where(new_slot, k_new[:, None], k_cache)
    v_cache = jnp.where(new_slot, v_new[:, None], v_cache)
    live_slot = (lengths[:, None] - jnp.remainder(lengths[:, None] - slot_ids[None, :], WINDOW)) >= 0
    attn_out = lax.map(attend_row, (q_heads, k_cache, v_cache, live_slot))
    resid_out = (resid_f32 + jnp.dot(attn_out, w_out, preferred_element_type=jnp.float32)).astype(jnp.bfloat16)
    return (resid_out, k_cache, v_cache)
```

```python
import functools

import jax
import jax.numpy as jnp
from jax import lax
from jax.experimental import pallas as pl
from jax.experimental.pallas import tpu as pltpu
from jax.sharding import PartitionSpec as P

WINDOW = 4096
THETA = 10000.0
EPS = 1e-5
GROUP = 32
BLOCK = 256
WRAP = 256


def rotate(heads, positions):
    head_dim = heads.shape[-1]
    half_dim = head_dim // 2
    inv_freq = THETA ** (-2.0 * jnp.arange(half_dim, dtype=jnp.float32) / head_dim)
    angles = positions.astype(jnp.float32).reshape(positions.shape + (1,) * (heads.ndim - 1)) * inv_freq
    cos_part = jnp.cos(angles)
    sin_part = jnp.sin(angles)
    first_half = heads[..., :half_dim].astype(jnp.float32)
    second_half = heads[..., half_dim:].astype(jnp.float32)
    return jnp.concatenate([first_half * cos_part - second_half * sin_part, second_half * cos_part + first_half * sin_part], axis=-1).astype(jnp.bfloat16)


def interleave_kernel(first_slot, has_prev, *refs):
    len_ref, perm_ref, new_ref = refs[:3]
    head_refs = refs[3:11]
    out_ref = refs[-1]
    row_len = len_ref[0]
    new_slot = lax.rem(row_len, WINDOW)
    rows = GROUP * 8
    block_slot = first_slot + pl.program_id(0) * BLOCK
    slot_of_row = lax.broadcasted_iota(jnp.int32, (rows, 128), 0) // 8
    for pair in range(BLOCK // (2 * GROUP)):
        parts = []
        for half in range(2):
            at = (2 * pair + half) * GROUP
            parts.append(jnp.concatenate([ref[at:at + GROUP, :] for ref in head_refs], axis=0))
        mixed = jnp.dot(perm_ref[...], jnp.concatenate(parts, axis=1), preferred_element_type=jnp.float32)
        for half in range(2):
            at = (2 * pair + half) * GROUP
            slots = slot_of_row + (block_slot + at)
            held = jnp.where(slots < row_len, mixed[:, half * 128:(half + 1) * 128], 0.0)
            held = jnp.where(slots == new_slot, new_ref[...], held)
            out_ref[at * 8:(at + GROUP) * 8, :] = held.astype(jnp.bfloat16)


def interleave(first_slot, heads, row_len, perm, new_rows, cache):
    num_slots = heads[0].shape[0]
    head_spec = pl.BlockSpec((BLOCK, 128), lambda i: (i, 0))
    in_specs = [pl.BlockSpec(memory_space=pltpu.SMEM), pl.BlockSpec((GROUP * 8, GROUP * 8), lambda i: (0, 0)), pl.BlockSpec((GROUP * 8, 128), lambda i: (0, 0))] + [head_spec] * 8
    args = [row_len, perm, new_rows, *heads]
    aliases = {}
    if cache is not None:
        in_specs.append(pl.BlockSpec(memory_space=pl.ANY))
        aliases = {len(args): 0}
        args.append(cache)
    return pl.pallas_call(
        functools.partial(interleave_kernel, first_slot, cache is not None),
        grid=(num_slots // BLOCK,),
        out_shape=jax.ShapeDtypeStruct((WINDOW * 8, 128), jnp.bfloat16),
        in_specs=in_specs,
        out_specs=pl.BlockSpec((BLOCK * 8, 128), lambda i: (first_slot // BLOCK + i, 0)),
        input_output_aliases=aliases,
        compiler_params=pltpu.CompilerParams(vmem_limit_bytes=16 * 1024 * 1024),
        cost_estimate=pl.CostEstimate(flops=num_slots * 8 * 256 * 128 * 2, bytes_accessed=num_slots * 8 * 128 * 4, transcendentals=0),
    )(*args)


def solution(mesh):
    head_spec = P('dp', None, 'sh', None)
    row_spec = P(('dp', 'sh'))
    full_spec = P(None, None)
    peers = mesh.shape['sh']
    order = (6, 4, 2, 7, 5, 3, 1)

    def swap(value, offset):
        return lax.ppermute(value, 'sh', [(i, i ^ offset) for i in range(peers)])

    def exchange(table, me):
        got = [lax.dynamic_slice_in_dim(table, me ^ offset, 1) for offset in range(peers)]
        got = [got[0]] + [swap(got[offset], offset) for offset in range(1, peers)]
        return jnp.take(jnp.concatenate(got, axis=0), me ^ jnp.arange(peers), axis=0)

    def send_chunk(prefill, lengths, me, first_slot, num_slots):
        own = []
        for offset in (0,) + order:
            row = me ^ offset
            piece = lax.dynamic_slice(prefill, (row, first_slot, 0), (1, num_slots, 128))
            if first_slot == 0:
                late = lax.dynamic_slice(prefill, (row, WINDOW, 0), (1, num_slots, 128))
                late_pos = WINDOW + jnp.arange(num_slots, dtype=jnp.int32)
                piece = jnp.where((late_pos < lengths[row])[None, :, None], late, piece)
            own.append((offset, piece))
        return own

    def per_device(k_prefill, v_prefill, lengths, residual, norm_gain, w_query, w_key, w_value, w_out):
        me = lax.axis_index('sh')
        seq_len = k_prefill.shape[1]
        head_dim = k_prefill.shape[3]
        k_mine = k_prefill.reshape(peers, seq_len, head_dim)
        v_mine = v_prefill.reshape(peers, seq_len, head_dim)
        my_len = lax.dynamic_slice_in_dim(lengths, me, 1)

        chunks = [(WRAP, 1280), (WRAP + 1280, 1280), (WRAP + 2560, 1280), (0, WRAP)]
        received = {}

        def start(name, prefill, chunk):
            pieces = send_chunk(prefill, lengths, me, *chunk)
            heads = {}
            for offset, piece in pieces:
                heads[offset] = piece if offset == 0 else swap(piece, offset)
            received[name, chunk[0]] = [heads[offset].reshape(chunk[1], head_dim) for offset in range(peers)]

        for chunk in chunks:
            start('k', k_mine, chunk)

        resid_f32 = residual.astype(jnp.float32)
        inv_rms = lax.rsqrt(jnp.mean(resid_f32 * resid_f32, axis=-1, keepdims=True) + EPS)
        normed = (resid_f32 * inv_rms * norm_gain.astype(jnp.float32)).astype(jnp.bfloat16)
        q_heads = jnp.dot(normed, w_query, preferred_element_type=jnp.float32).astype(jnp.bfloat16).reshape(1, -1, head_dim)
        k_new = jnp.dot(normed, w_key, preferred_element_type=jnp.float32).astype(jnp.bfloat16).reshape(1, peers, head_dim)
        v_new = jnp.dot(normed, w_value, preferred_element_type=jnp.float32).astype(jnp.bfloat16).reshape(1, peers, head_dim)
        q_heads = rotate(q_heads, my_len)
        k_new = rotate(k_new, my_len)
        q_group = q_heads.shape[1] // peers

        table = jnp.concatenate([q_heads.reshape(peers, q_group, head_dim), k_new.reshape(peers, 1, head_dim), v_new.reshape(peers, 1, head_dim)], axis=1)
        qkv = exchange(table.reshape(peers, -1), me).reshape(peers, q_group + 2, head_dim)
        q_all, k_all, v_all = qkv[:, :q_group], qkv[:, q_group:q_group + 1], qkv[:, q_group + 1:]
        positions = jnp.arange(seq_len, dtype=jnp.int32)[None, :]
        live = (positions < lengths[:, None]) & (positions > lengths[:, None] - WINDOW)
        scale = 1.0 / head_dim ** 0.5
        scores = jnp.einsum('bgd,bsd->bgs', q_all, k_mine, preferred_element_type=jnp.float32) / head_dim ** 0.5
        scores = jnp.where(live[:, None, :], scores, -jnp.inf)
        new_score = jnp.sum(q_all.astype(jnp.float32) * k_all.astype(jnp.float32), axis=-1, keepdims=True) / head_dim ** 0.5
        top = jnp.maximum(jnp.max(scores, axis=-1, keepdims=True), new_score)
        exp_scores = jnp.exp(scores - top)
        exp_new = jnp.exp(new_score - top)
        total = jnp.sum(exp_scores, axis=-1, keepdims=True) + exp_new
        weights = (exp_scores / total).astype(jnp.bfloat16)
        new_weight = (exp_new / total).astype(jnp.bfloat16)
        mixed = jnp.einsum('bgs,bsd->bgd', weights, v_mine, preferred_element_type=jnp.float32)
        mixed = (mixed + new_weight.astype(jnp.float32) * v_all.astype(jnp.float32)).astype(jnp.bfloat16)
        attn_out = exchange(mixed.reshape(peers, -1), me).reshape(1, -1)

        for chunk in chunks:
            start('v', v_mine, chunk)

        resid_out = (resid_f32 + jnp.dot(attn_out, w_out, preferred_element_type=jnp.float32)).astype(jnp.bfloat16)

        out_row = jnp.arange(GROUP * 8, dtype=jnp.int32)[:, None]
        in_row = jnp.arange(GROUP * 8, dtype=jnp.int32)[None, :]
        perm = ((out_row // 8 == in_row % GROUP) & (out_row % 8 == (in_row // GROUP) ^ me)).astype(jnp.bfloat16)
        caches = []
        for name, new in (('k', k_new), ('v', v_new)):
            new_rows = jnp.tile(new[0].astype(jnp.float32), (GROUP, 1))
            cache = None
            for chunk in chunks:
                cache = interleave(chunk[0], received[name, chunk[0]], my_len, perm, new_rows, cache)
            caches.append(cache.reshape(1, WINDOW, peers, head_dim))
        return resid_out, caches[0], caches[1]

    return jax.shard_map(per_device, mesh=mesh, in_specs=(head_spec, head_spec, P('dp'), P(('dp', 'sh'), None), P(None), full_spec, full_spec, full_spec, full_spec), out_specs=(P(('dp', 'sh'), None), row_spec, row_spec), check_vma=False)
```

```python
import functools

import jax
import jax.numpy as jnp
from jax import lax
from jax.experimental import pallas as pl
from jax.experimental.pallas import tpu as pltpu
from jax.sharding import PartitionSpec as P


WINDOW = 4096
THETA = 10000.0
EPS = 1e-5
GROUP = 32
BLOCK = 256
K_CHUNKS = ((256, 1280), (1536, 1280), (2816, 1280), (0, 256))
V_CHUNKS = ((256, 1792), (2048, 1280), (3328, 768), (0, 256))


def rotate(heads, positions):
    head_dim = heads.shape[-1]
    half_dim = head_dim // 2
    inv_freq = THETA ** (-2.0 * jnp.arange(half_dim, dtype=jnp.float32) / head_dim)
    angles = positions.astype(jnp.float32).reshape(positions.shape + (1,) * (heads.ndim - 1)) * inv_freq
    cos_part = jnp.cos(angles)
    sin_part = jnp.sin(angles)
    first_half = heads[..., :half_dim].astype(jnp.float32)
    second_half = heads[..., half_dim:].astype(jnp.float32)
    return jnp.concatenate([first_half * cos_part - second_half * sin_part, second_half * cos_part + first_half * sin_part], axis=-1).astype(jnp.bfloat16)


def interleave_kernel(first_slot, *refs):
    len_ref, perm_ref, new_ref = refs[:3]
    head_refs = refs[3:11]
    out_ref = refs[-1]
    row_len = len_ref[0]
    new_slot = lax.rem(row_len, WINDOW)
    rows = GROUP * 8
    block_slot = first_slot + pl.program_id(0) * BLOCK
    slot_of_row = lax.broadcasted_iota(jnp.int32, (rows, 128), 0) // 8
    for pair in range(BLOCK // (2 * GROUP)):
        parts = []
        for half in range(2):
            at = (2 * pair + half) * GROUP
            parts.append(jnp.concatenate([ref[at:at + GROUP, :] for ref in head_refs], axis=0))
        mixed = jnp.dot(perm_ref[...], jnp.concatenate(parts, axis=1), preferred_element_type=jnp.float32)
        for half in range(2):
            at = (2 * pair + half) * GROUP
            slots = slot_of_row + (block_slot + at)
            held = jnp.where(slots < row_len, mixed[:, half * 128:(half + 1) * 128], 0.0)
            held = jnp.where(slots == new_slot, new_ref[...], held)
            out_ref[at * 8:(at + GROUP) * 8, :] = held.astype(jnp.bfloat16)


def interleave(first_slot, heads, row_len, perm, new_rows, cache):
    num_slots = heads[0].shape[0]
    head_spec = pl.BlockSpec((BLOCK, 128), lambda i: (i, 0))
    in_specs = [pl.BlockSpec(memory_space=pltpu.SMEM), pl.BlockSpec((GROUP * 8, GROUP * 8), lambda i: (0, 0)), pl.BlockSpec((GROUP * 8, 128), lambda i: (0, 0))] + [head_spec] * 8
    args = [row_len, perm, new_rows, *heads]
    aliases = {}
    if cache is not None:
        in_specs.append(pl.BlockSpec(memory_space=pl.ANY))
        aliases = {len(args): 0}
        args.append(cache)
    return pl.pallas_call(
        functools.partial(interleave_kernel, first_slot),
        grid=(num_slots // BLOCK,),
        out_shape=jax.ShapeDtypeStruct((WINDOW * 8, 128), jnp.bfloat16),
        in_specs=in_specs,
        out_specs=pl.BlockSpec((BLOCK * 8, 128), lambda i: (first_slot // BLOCK + i, 0)),
        input_output_aliases=aliases,
        compiler_params=pltpu.CompilerParams(vmem_limit_bytes=16 * 1024 * 1024),
        cost_estimate=pl.CostEstimate(flops=num_slots * 8 * 256 * 128 * 2, bytes_accessed=num_slots * 8 * 128 * 4, transcendentals=0),
    )(*args)


def solution(mesh):
    head_spec = P('dp', None, 'sh', None)
    row_spec = P(('dp', 'sh'))
    full_spec = P(None, None)
    peers = mesh.shape['sh']
    order = (6, 4, 2, 7, 5, 3, 1)

    def swap(value, offset):
        return lax.ppermute(value, 'sh', [(i, i ^ offset) for i in range(peers)])

    def exchange(table, me):
        got = [lax.dynamic_slice_in_dim(table, me ^ offset, 1) for offset in range(peers)]
        return [got[0]] + [swap(got[offset], offset) for offset in range(1, peers)]

    def by_device(got, me):
        return jnp.take(jnp.concatenate(got, axis=0), me ^ jnp.arange(peers), axis=0)

    def send_chunk(prefill, lengths, me, first_slot, num_slots):
        pieces = []
        for offset in order + (0,):
            row = me ^ offset
            piece = lax.dynamic_slice(prefill, (row, first_slot, 0), (1, num_slots, prefill.shape[2]))
            if first_slot == 0:
                late = lax.dynamic_slice(prefill, (row, WINDOW, 0), (1, num_slots, prefill.shape[2]))
                late_pos = WINDOW + jnp.arange(num_slots, dtype=jnp.int32)
                piece = jnp.where((late_pos < lengths[row])[None, :, None], late, piece)
            pieces.append(piece)
        return pieces

    def per_device(k_prefill, v_prefill, lengths, residual, norm_gain, w_query, w_key, w_value, w_out):
        me = lax.axis_index('sh')
        seq_len = k_prefill.shape[1]
        head_dim = k_prefill.shape[3]
        mine = {'k': k_prefill.reshape(peers, seq_len, head_dim), 'v': v_prefill.reshape(peers, seq_len, head_dim)}
        my_len = lax.dynamic_slice_in_dim(lengths, me, 1)
        received = {}

        def start(name, chunk, after=None, before=None):
            prefill = mine[name]
            if after is not None:
                prefill, after = lax.optimization_barrier((prefill, after))
            pieces = send_chunk(prefill, lengths, me, *chunk)
            pieces, before = lax.optimization_barrier((pieces, before))
            heads = {0: pieces[-1]}
            for offset, piece in zip(order, pieces):
                heads[offset] = swap(piece, offset)
            received[name, chunk[0]] = [heads[offset].reshape(chunk[1], head_dim) for offset in range(peers)]
            return before, after

        out_row = jnp.arange(GROUP * 8, dtype=jnp.int32)[:, None]
        in_row = jnp.arange(GROUP * 8, dtype=jnp.int32)[None, :]
        perm = ((out_row // 8 == in_row % GROUP) & (out_row % 8 == (in_row // GROUP) ^ me)).astype(jnp.bfloat16)
        caches = {'k': None, 'v': None}
        new_rows = {}

        def store(name, chunk):
            caches[name] = interleave(chunk[0], received[name, chunk[0]], my_len, perm, new_rows[name], caches[name])

        residual, _ = start('k', K_CHUNKS[0], before=residual)
        residual, _ = start('k', K_CHUNKS[1], after=residual, before=residual)

        resid_f32 = residual.astype(jnp.float32)
        inv_rms = lax.rsqrt(jnp.mean(resid_f32 * resid_f32, axis=-1, keepdims=True) + EPS)
        normed = (resid_f32 * inv_rms * norm_gain.astype(jnp.float32)).astype(jnp.bfloat16)
        q_heads = jnp.dot(normed, w_query, preferred_element_type=jnp.float32).astype(jnp.bfloat16).reshape(1, -1, head_dim)
        k_new = jnp.dot(normed, w_key, preferred_element_type=jnp.float32).astype(jnp.bfloat16).reshape(1, peers, head_dim)
        v_new = jnp.dot(normed, w_value, preferred_element_type=jnp.float32).astype(jnp.bfloat16).reshape(1, peers, head_dim)
        q_heads = rotate(q_heads, my_len)
        k_new = rotate(k_new, my_len)
        q_group = q_heads.shape[1] // peers
        for name, new in (('k', k_new), ('v', v_new)):
            new_rows[name] = jnp.tile(new[0].astype(jnp.float32), (GROUP, 1))

        table = jnp.concatenate([q_heads.reshape(peers, q_group, head_dim), k_new.reshape(peers, 1, head_dim), v_new.reshape(peers, 1, head_dim)], axis=1).reshape(peers, -1)
        qkv = by_device(exchange(table, me), me)
        start('k', K_CHUNKS[2], after=table)
        qkv, _ = start('v', V_CHUNKS[0], after=qkv, before=qkv)
        qkv = qkv.reshape(peers, q_group + 2, head_dim)
        q_all, k_all, v_all = qkv[:, :q_group], qkv[:, q_group:q_group + 1], qkv[:, q_group + 1:]
        positions = jnp.arange(seq_len, dtype=jnp.int32)[None, :]
        live = (positions < lengths[:, None]) & (positions > lengths[:, None] - WINDOW)
        scores = jnp.einsum('bgd,bsd->bgs', q_all, mine['k'], preferred_element_type=jnp.float32) / head_dim ** 0.5
        scores = jnp.where(live[:, None, :], scores, -jnp.inf)
        top_old = jnp.max(scores, axis=-1, keepdims=True)
        new_score = jnp.sum(q_all.astype(jnp.float32) * k_all.astype(jnp.float32), axis=-1, keepdims=True) / head_dim ** 0.5
        top = jnp.maximum(top_old, new_score)
        exp_scores = jnp.exp(scores - top)
        exp_new = jnp.exp(new_score - top)
        total = jnp.sum(exp_scores, axis=-1, keepdims=True) + exp_new
        weights = (exp_scores / total).astype(jnp.bfloat16)
        new_weight = lax.reduce_precision(exp_new / total, 8, 7)
        mixed = jnp.einsum('bgs,bsd->bgd', weights, mine['v'], preferred_element_type=jnp.float32)
        mixed = (mixed + new_weight * v_all.astype(jnp.float32)).astype(jnp.bfloat16).reshape(peers, -1)
        attn_parts = exchange(mixed, me)

        received['k', K_CHUNKS[0][0]], _ = lax.optimization_barrier((received['k', K_CHUNKS[0][0]], mixed))
        store('k', K_CHUNKS[0])
        store('k', K_CHUNKS[1])
        _, caches['k'] = start('v', V_CHUNKS[1], after=caches['k'])
        caches['k'], _ = start('k', K_CHUNKS[3], after=caches['k'], before=caches['k'])
        store('k', K_CHUNKS[2])
        attn_parts, caches['k'] = lax.optimization_barrier((attn_parts, caches['k']))
        attn_out = by_device(attn_parts, me).reshape(1, -1)
        resid_out = (resid_f32 + jnp.dot(attn_out, w_out, preferred_element_type=jnp.float32)).astype(jnp.bfloat16)
        for chunk in V_CHUNKS[2:]:
            _, caches['k'] = start('v', chunk, after=caches['k'])
        store('v', V_CHUNKS[0])
        store('k', K_CHUNKS[3])
        for chunk in V_CHUNKS[1:]:
            store('v', chunk)
        shape = (1, WINDOW, peers, head_dim)
        return resid_out, caches['k'].reshape(shape), caches['v'].reshape(shape)

    return jax.shard_map(per_device, mesh=mesh, in_specs=(head_spec, head_spec, P('dp'), P(('dp', 'sh'), None), P(None), full_spec, full_spec, full_spec, full_spec), out_specs=(P(('dp', 'sh'), None), row_spec, row_spec), check_vma=False)
```

```python
import functools

import jax
import jax.numpy as jnp
from jax import lax
from jax.experimental import pallas as pl
from jax.experimental.pallas import tpu as pltpu
from jax.sharding import PartitionSpec as P


WINDOW = 4096
THETA = 10000.0
EPS = 1e-5
PEERS = 8
GROUP = 32
WRAP = 256
CHUNKS = ((256, 512), (768, 1280), (2048, 1280), (3328, 512), (3840, 256))
BLOCK = 256
ORDER = (6, 4, 2, 7, 5, 3, 1)
MIB = 1024 * 1024


def rotate(heads, positions):
    head_dim = heads.shape[-1]
    half_dim = head_dim // 2
    inv_freq = THETA ** (-2.0 * jnp.arange(half_dim, dtype=jnp.float32) / head_dim)
    angles = positions.astype(jnp.float32).reshape(positions.shape + (1,) * (heads.ndim - 1)) * inv_freq
    cos_part = jnp.cos(angles)
    sin_part = jnp.sin(angles)
    first_half = heads[..., :half_dim].astype(jnp.float32)
    second_half = heads[..., half_dim:].astype(jnp.float32)
    return jnp.concatenate([first_half * cos_part - second_half * sin_part, second_half * cos_part + first_half * sin_part], axis=-1).astype(jnp.bfloat16)


def pack_kernel(first, count, me_ref, k_ref, v_ref, *refs):
    outs = refs[:len(ORDER)]
    held, in_sems, out_sems = refs[len(ORDER):]
    me = me_ref[0]
    reads = []
    for at, offset in enumerate(ORDER):
        for kv, src in enumerate((k_ref, v_ref)):
            reads.append(pltpu.make_async_copy(src.at[me ^ offset, pl.ds(first, count)], held.at[at, kv], in_sems.at[at, kv]))
            reads[-1].start()
    writes = []
    for at, out in enumerate(outs):
        reads[2 * at].wait()
        reads[2 * at + 1].wait()
        writes.append(pltpu.make_async_copy(held.at[at], out, out_sems.at[at]))
        writes[-1].start()
    for write in writes:
        write.wait()


def pack(first, count, me, k_mine, v_mine):
    dim = k_mine.shape[2]
    piece = jax.ShapeDtypeStruct((2, count, dim), jnp.bfloat16)
    return pl.pallas_call(
        functools.partial(pack_kernel, first, count),
        out_shape=[piece] * len(ORDER),
        in_specs=[pl.BlockSpec(memory_space=pltpu.SMEM)] + [pl.BlockSpec(memory_space=pltpu.HBM)] * 2,
        out_specs=[pl.BlockSpec(memory_space=pltpu.HBM)] * len(ORDER),
        scratch_shapes=[pltpu.VMEM((len(ORDER), 2, count, dim), jnp.bfloat16), pltpu.SemaphoreType.DMA((len(ORDER), 2)), pltpu.SemaphoreType.DMA((len(ORDER),))],
        compiler_params=pltpu.CompilerParams(vmem_limit_bytes=12 * MIB),
        cost_estimate=pl.CostEstimate(flops=0, bytes_accessed=len(ORDER) * 4 * count * dim * 2, transcendentals=0),
    )(me, k_mine, v_mine)


def wrap_kernel(me_ref, len_ref, k_ref, k_late_ref, v_ref, v_late_ref, *outs):
    me = me_ref[0]
    slots = lax.broadcasted_iota(jnp.int32, (WRAP, 128), 0)
    for out, offset in zip(outs, ORDER + (0,)):
        row = me ^ offset
        late = slots + WINDOW < len_ref[row]
        for kv, (base_ref, late_ref) in enumerate(((k_ref, k_late_ref), (v_ref, v_late_ref))):
            out[kv] = jnp.where(late, late_ref[row].astype(jnp.float32), base_ref[row].astype(jnp.float32)).astype(jnp.bfloat16)


def wrap_pack(me, lengths, k_mine, v_mine):
    rows, _, dim = k_mine.shape
    base = pl.BlockSpec((rows, WRAP, dim), lambda i: (0, 0, 0))
    late = pl.BlockSpec((rows, WRAP, dim), lambda i: (0, WINDOW // WRAP, 0))
    piece = jax.ShapeDtypeStruct((2, WRAP, dim), jnp.bfloat16)
    return pl.pallas_call(
        wrap_kernel,
        grid=(1,),
        out_shape=[piece] * (len(ORDER) + 1),
        out_specs=[pl.BlockSpec((2, WRAP, dim), lambda i: (0, 0, 0))] * (len(ORDER) + 1),
        in_specs=[pl.BlockSpec(memory_space=pltpu.SMEM)] * 2 + [base, late, base, late],
        compiler_params=pltpu.CompilerParams(vmem_limit_bytes=16 * MIB),
        cost_estimate=pl.CostEstimate(flops=rows * 8 * WRAP * dim, bytes_accessed=rows * 6 * WRAP * dim * 2, transcendentals=0),
    )(me, lengths, k_mine, k_mine, v_mine, v_mine)


def interleave_kernel(first, count, block, has_own, num_alias, me_ref, len_ref, new_ref, *refs):
    num_own = 2 if has_own else 1
    own = refs[:num_own]
    pieces = refs[num_own:num_own + len(ORDER)]
    k_out, v_out, held, mixed, in_sems, out_sems = refs[num_own + len(ORDER) + num_alias:]
    tiles = count // block
    me = me_ref[0]
    row_len = len_ref[0]
    new_slot = lax.rem(row_len, WINDOW)
    outs = (k_out, v_out)

    def read(tile, kv, offset):
        at = pl.multiple_of(tile * block, block)
        if offset:
            src = pieces[ORDER.index(offset)].at[kv, pl.ds(at, block)]
        elif has_own:
            src = own[kv].at[me, pl.ds(first + at, block)]
        else:
            src = own[0].at[kv, pl.ds(at, block)]
        return pltpu.make_async_copy(src, held.at[tile, kv, me ^ offset], in_sems.at[tile, kv, offset])

    def write(tile, kv):
        at = pl.multiple_of((first + tile * block) * PEERS, block * PEERS)
        return pltpu.make_async_copy(mixed.at[tile, kv], outs[kv].at[pl.ds(at, block * PEERS)], out_sems.at[tile, kv])

    @pl.loop(0, tiles)
    def _(tile):
        for kv in range(2):
            for offset in range(PEERS):
                read(tile, kv, offset).start()

    @pl.loop(0, tiles)
    def _(tile):
        start = first + tile * block
        plain = (start + block <= row_len) & ((new_slot < start) | (new_slot >= start + block))
        for kv in range(2):
            for offset in range(PEERS):
                read(tile, kv, offset).wait()

            def group(at):
                return jnp.swapaxes(held[tile, kv, :, at:at + GROUP, :], 0, 1).reshape(GROUP * PEERS, -1)

            @pl.when(plain)
            def _():
                for at in range(0, block, GROUP):
                    mixed[tile, kv, at * PEERS:(at + GROUP) * PEERS, :] = group(at)

            @pl.when(jnp.logical_not(plain))
            def _():
                new = jnp.concatenate([new_ref[kv]] * GROUP, axis=0)
                slot_of_row = lax.broadcasted_iota(jnp.int32, new.shape, 0) // PEERS
                for at in range(0, block, GROUP):
                    slots = slot_of_row + (start + at)
                    rows = jnp.where(slots < row_len, group(at).astype(jnp.float32), 0.0)
                    rows = jnp.where(slots == new_slot, new, rows)
                    mixed[tile, kv, at * PEERS:(at + GROUP) * PEERS, :] = rows.astype(jnp.bfloat16)

            write(tile, kv).start()

    @pl.loop(0, tiles)
    def _(tile):
        for kv in range(2):
            write(tile, kv).wait()


def interleave(first, me, row_len, new, own, pieces, caches):
    count, dim = pieces[0].shape[1:]
    block = min(count, BLOCK)
    tiles = count // block
    cache = jax.ShapeDtypeStruct((WINDOW * PEERS, dim), jnp.bfloat16)
    any_spec = pl.BlockSpec(memory_space=pltpu.HBM)
    args = [me, row_len, new, *own, *pieces]
    in_specs = [pl.BlockSpec(memory_space=pltpu.SMEM)] * 2 + [pl.BlockSpec(memory_space=pltpu.VMEM)] + [any_spec] * (len(own) + len(pieces))
    aliases = {}
    if caches is not None:
        aliases = {len(args): 0, len(args) + 1: 1}
        args += caches
        in_specs += [any_spec] * 2
    return pl.pallas_call(
        functools.partial(interleave_kernel, first, count, block, len(own) == 2, len(aliases)),
        out_shape=[cache, cache],
        in_specs=in_specs,
        out_specs=[any_spec] * 2,
        input_output_aliases=aliases,
        scratch_shapes=[
            pltpu.VMEM((tiles, 2, PEERS, block, dim), jnp.bfloat16),
            pltpu.VMEM((tiles, 2, block * PEERS, dim), jnp.bfloat16),
            pltpu.SemaphoreType.DMA((tiles, 2, PEERS)),
            pltpu.SemaphoreType.DMA((tiles, 2)),
        ],
        compiler_params=pltpu.CompilerParams(vmem_limit_bytes=16 * MIB),
        cost_estimate=pl.CostEstimate(flops=count * 64 * dim, bytes_accessed=count * PEERS * dim * 8, transcendentals=0),
    )(*args)


def solution(mesh):
    head_spec = P('dp', None, 'sh', None)
    row_spec = P(('dp', 'sh'))
    full_spec = P(None, None)

    def swap(value, offset):
        return lax.ppermute(value, 'sh', [(i, i ^ offset) for i in range(PEERS)])

    def exchange(table, me):
        got = [lax.dynamic_slice_in_dim(table, me ^ offset, 1) for offset in range(PEERS)]
        return [got[0]] + [swap(got[offset], offset) for offset in range(1, PEERS)]

    def by_device(got, me):
        return jnp.take(jnp.concatenate(got, axis=0), me ^ jnp.arange(PEERS), axis=0)

    def per_device(k_prefill, v_prefill, lengths, residual, norm_gain, w_query, w_key, w_value, w_out):
        me = lax.axis_index('sh')
        me_vec = me.reshape(1).astype(jnp.int32)
        seq_len = k_prefill.shape[1]
        head_dim = k_prefill.shape[3]
        k_mine = k_prefill.reshape(PEERS, seq_len, head_dim)
        v_mine = v_prefill.reshape(PEERS, seq_len, head_dim)
        my_len = lax.dynamic_slice_in_dim(lengths, me, 1)
        received = {}

        def send(first, pieces):
            received[first] = [swap(piece, offset) for piece, offset in zip(pieces, ORDER)]

        def start(chunk, after=None, before=None):
            place = me_vec
            if after is not None:
                place, after = lax.optimization_barrier((place, after))
            pieces = pack(*chunk, place, k_mine, v_mine)
            pieces, before = lax.optimization_barrier((pieces, before))
            send(chunk[0], pieces)
            return after, before

        _, residual = start(CHUNKS[0], before=residual)
        _, residual = start(CHUNKS[1], after=residual, before=residual)

        resid_f32 = residual.astype(jnp.float32)
        inv_rms = lax.rsqrt(jnp.mean(resid_f32 * resid_f32, axis=-1, keepdims=True) + EPS)
        normed = (resid_f32 * inv_rms * norm_gain.astype(jnp.float32)).astype(jnp.bfloat16)
        q_heads = jnp.dot(normed, w_query, preferred_element_type=jnp.float32).astype(jnp.bfloat16).reshape(1, -1, head_dim)
        k_new = jnp.dot(normed, w_key, preferred_element_type=jnp.float32).astype(jnp.bfloat16).reshape(1, PEERS, head_dim)
        v_new = jnp.dot(normed, w_value, preferred_element_type=jnp.float32).astype(jnp.bfloat16).reshape(1, PEERS, head_dim)
        q_heads = rotate(q_heads, my_len)
        k_new = rotate(k_new, my_len)
        q_group = q_heads.shape[1] // PEERS
        new = jnp.concatenate([k_new, v_new], axis=0).astype(jnp.float32)

        table = jnp.concatenate([q_heads.reshape(PEERS, q_group, head_dim), k_new.reshape(PEERS, 1, head_dim), v_new.reshape(PEERS, 1, head_dim)], axis=1).reshape(PEERS, -1)
        qkv_parts = exchange(table, me)
        _, table = start(CHUNKS[2], after=table, before=table)
        wrap_place, _ = lax.optimization_barrier((me_vec, table))
        wrapped = wrap_pack(wrap_place, lengths, k_mine, v_mine)
        send(0, wrapped[:-1])
        qkv = by_device(qkv_parts, me).reshape(PEERS, q_group + 2, head_dim)
        q_all, k_all, v_all = qkv[:, :q_group], qkv[:, q_group:q_group + 1], qkv[:, q_group + 1:]
        positions = jnp.arange(seq_len, dtype=jnp.int32)[None, :]
        live = (positions < lengths[:, None]) & (positions > lengths[:, None] - WINDOW)
        scores = jnp.einsum('bgd,bsd->bgs', q_all, k_mine, preferred_element_type=jnp.float32) / head_dim ** 0.5
        scores = jnp.where(live[:, None, :], scores, -jnp.inf)
        top_old = jnp.max(scores, axis=-1, keepdims=True)
        new_score = jnp.sum(q_all.astype(jnp.float32) * k_all.astype(jnp.float32), axis=-1, keepdims=True) / head_dim ** 0.5
        top = jnp.maximum(top_old, new_score)
        exp_scores = jnp.exp(scores - top)
        exp_new = jnp.exp(new_score - top)
        total = jnp.sum(exp_scores, axis=-1, keepdims=True) + exp_new
        weights = (exp_scores / total).astype(jnp.bfloat16)
        new_weight = lax.reduce_precision(exp_new / total, 8, 7)
        mixed = jnp.einsum('bgs,bsd->bgd', weights, v_mine, preferred_element_type=jnp.float32)
        mixed = (mixed + new_weight * v_all.astype(jnp.float32)).astype(jnp.bfloat16).reshape(PEERS, -1)
        attn_parts = exchange(mixed, me)

        place, _ = lax.optimization_barrier((me_vec, mixed))
        caches = None

        def store(first, caches):
            own = [wrapped[-1]] if first == 0 else [k_mine, v_mine]
            return interleave(first, place, my_len, new, own, received[first], caches)

        caches = store(CHUNKS[0][0], caches)
        caches = store(CHUNKS[1][0], caches)
        caches, caches = start(CHUNKS[3], after=caches, before=caches)
        caches, caches = start(CHUNKS[4], after=caches, before=caches)
        caches = store(CHUNKS[2][0], caches)
        attn_parts, caches = lax.optimization_barrier((attn_parts, caches))
        attn_out = by_device(attn_parts, me).reshape(1, -1)
        resid_out = (resid_f32 + jnp.dot(attn_out, w_out, preferred_element_type=jnp.float32)).astype(jnp.bfloat16)
        for first in (0, CHUNKS[3][0], CHUNKS[4][0]):
            caches = store(first, caches)
        shape = (1, WINDOW, PEERS, head_dim)
        return resid_out, caches[0].reshape(shape), caches[1].reshape(shape)

    return jax.shard_map(per_device, mesh=mesh, in_specs=(head_spec, head_spec, P('dp'), P(('dp', 'sh'), None), P(None), full_spec, full_spec, full_spec, full_spec), out_specs=(P(('dp', 'sh'), None), row_spec, row_spec), check_vma=False)
```

```python
import functools

import jax
import jax.numpy as jnp
from jax import lax
from jax.experimental import pallas as pl
from jax.experimental.pallas import tpu as pltpu
from jax.sharding import PartitionSpec as P


WINDOW = 4096
THETA = 10000.0
EPS = 1e-5
PEERS = 8
GROUP = 32
WRAP = 256
CHUNKS = ((256, 512), (768, 1280), (2048, 1280), (3328, 512), (3840, 256))
BLOCK = 256
ORDER = (6, 4, 2, 7, 5, 3, 1)
VMEM_LIMIT = 60 * 1024 * 1024


def rotate(heads, positions):
    head_dim = heads.shape[-1]
    half_dim = head_dim // 2
    inv_freq = THETA ** (-2.0 * jnp.arange(half_dim, dtype=jnp.float32) / head_dim)
    angles = positions.astype(jnp.float32).reshape(positions.shape + (1,) * (heads.ndim - 1)) * inv_freq
    cos_part = jnp.cos(angles)
    sin_part = jnp.sin(angles)
    first_half = heads[..., :half_dim].astype(jnp.float32)
    second_half = heads[..., half_dim:].astype(jnp.float32)
    return jnp.concatenate([first_half * cos_part - second_half * sin_part, second_half * cos_part + first_half * sin_part], axis=-1).astype(jnp.bfloat16)


def pack_kernel(first, count, me_ref, k_ref, v_ref, *refs):
    outs = refs[:len(ORDER)]
    held, in_sems, out_sems = refs[len(ORDER):]
    me = me_ref[0]
    reads = []
    for at, offset in enumerate(ORDER):
        for kv, src in enumerate((k_ref, v_ref)):
            reads.append(pltpu.make_async_copy(src.at[me ^ offset, pl.ds(first, count)], held.at[at, kv], in_sems.at[at, kv]))
            reads[-1].start()
    writes = []
    for at, out in enumerate(outs):
        reads[2 * at].wait()
        reads[2 * at + 1].wait()
        writes.append(pltpu.make_async_copy(held.at[at], out, out_sems.at[at]))
        writes[-1].start()
    for write in writes:
        write.wait()


def pack(first, count, me, k_mine, v_mine):
    dim = k_mine.shape[2]
    piece = jax.ShapeDtypeStruct((2, count, dim), jnp.bfloat16)
    return pl.pallas_call(
        functools.partial(pack_kernel, first, count),
        out_shape=[piece] * len(ORDER),
        in_specs=[pl.BlockSpec(memory_space=pltpu.SMEM)] + [pl.BlockSpec(memory_space=pltpu.HBM)] * 2,
        out_specs=[pl.BlockSpec(memory_space=pltpu.HBM)] * len(ORDER),
        scratch_shapes=[pltpu.VMEM((len(ORDER), 2, count, dim), jnp.bfloat16), pltpu.SemaphoreType.DMA((len(ORDER), 2)), pltpu.SemaphoreType.DMA((len(ORDER),))],
        compiler_params=pltpu.CompilerParams(vmem_limit_bytes=VMEM_LIMIT),
        cost_estimate=pl.CostEstimate(flops=0, bytes_accessed=len(ORDER) * 4 * count * dim * 2, transcendentals=0),
    )(me, k_mine, v_mine)


def wrap_kernel(me_ref, len_ref, k_ref, k_late_ref, v_ref, v_late_ref, *outs):
    me = me_ref[0]
    slots = lax.broadcasted_iota(jnp.int32, (WRAP, 128), 0)
    for out, offset in zip(outs, ORDER + (0,)):
        row = me ^ offset
        late = slots + WINDOW < len_ref[row]
        for kv, (base_ref, late_ref) in enumerate(((k_ref, k_late_ref), (v_ref, v_late_ref))):
            out[kv] = jnp.where(late, late_ref[row].astype(jnp.float32), base_ref[row].astype(jnp.float32)).astype(jnp.bfloat16)


def wrap_pack(me, lengths, k_mine, v_mine):
    rows, _, dim = k_mine.shape
    base = pl.BlockSpec((rows, WRAP, dim), lambda i: (0, 0, 0))
    late = pl.BlockSpec((rows, WRAP, dim), lambda i: (0, WINDOW // WRAP, 0))
    piece = jax.ShapeDtypeStruct((2, WRAP, dim), jnp.bfloat16)
    return pl.pallas_call(
        wrap_kernel,
        grid=(1,),
        out_shape=[piece] * (len(ORDER) + 1),
        out_specs=[pl.BlockSpec((2, WRAP, dim), lambda i: (0, 0, 0))] * (len(ORDER) + 1),
        in_specs=[pl.BlockSpec(memory_space=pltpu.SMEM)] * 2 + [base, late, base, late],
        compiler_params=pltpu.CompilerParams(vmem_limit_bytes=VMEM_LIMIT),
        cost_estimate=pl.CostEstimate(flops=rows * 8 * WRAP * dim, bytes_accessed=rows * 6 * WRAP * dim * 2, transcendentals=0),
    )(me, lengths, k_mine, k_mine, v_mine, v_mine)


def interleave_kernel(first, count, block, has_own, num_alias, me_ref, len_ref, new_ref, *refs):
    num_own = 2 if has_own else 1
    own = refs[:num_own]
    pieces = refs[num_own:num_own + len(ORDER)]
    k_out, v_out, held, mixed, in_sems, out_sems = refs[num_own + len(ORDER) + num_alias:]
    tiles = count // block
    me = me_ref[0]
    row_len = len_ref[0]
    new_slot = lax.rem(row_len, WINDOW)
    outs = (k_out, v_out)

    def read(tile, kv, offset):
        at = pl.multiple_of(tile * block, block)
        if offset:
            src = pieces[ORDER.index(offset)].at[kv, pl.ds(at, block)]
        elif has_own:
            src = own[kv].at[me, pl.ds(first + at, block)]
        else:
            src = own[0].at[kv, pl.ds(at, block)]
        return pltpu.make_async_copy(src, held.at[tile, kv, me ^ offset], in_sems.at[tile, kv, offset])

    def write(tile, kv):
        at = pl.multiple_of((first + tile * block) * PEERS, block * PEERS)
        return pltpu.make_async_copy(mixed.at[tile, kv], outs[kv].at[pl.ds(at, block * PEERS)], out_sems.at[tile, kv])

    @pl.loop(0, tiles)
    def _(tile):
        for kv in range(2):
            for offset in range(PEERS):
                read(tile, kv, offset).start()

    @pl.loop(0, tiles)
    def _(tile):
        start = first + tile * block
        plain = (start + block <= row_len) & ((new_slot < start) | (new_slot >= start + block))
        for kv in range(2):
            for offset in range(PEERS):
                read(tile, kv, offset).wait()

            def group(at):
                return jnp.swapaxes(held[tile, kv, :, at:at + GROUP, :], 0, 1).reshape(GROUP * PEERS, -1)

            @pl.when(plain)
            def _():
                for at in range(0, block, GROUP):
                    mixed[tile, kv, at * PEERS:(at + GROUP) * PEERS, :] = group(at)

            @pl.when(jnp.logical_not(plain))
            def _():
                new = jnp.concatenate([new_ref[kv]] * GROUP, axis=0)
                slot_of_row = lax.broadcasted_iota(jnp.int32, new.shape, 0) // PEERS
                for at in range(0, block, GROUP):
                    slots = slot_of_row + (start + at)
                    rows = jnp.where(slots < row_len, group(at).astype(jnp.float32), 0.0)
                    rows = jnp.where(slots == new_slot, new, rows)
                    mixed[tile, kv, at * PEERS:(at + GROUP) * PEERS, :] = rows.astype(jnp.bfloat16)

            write(tile, kv).start()

    @pl.loop(0, tiles)
    def _(tile):
        for kv in range(2):
            write(tile, kv).wait()


def interleave(first, me, row_len, new, own, pieces, caches):
    count, dim = pieces[0].shape[1:]
    block = min(count, BLOCK)
    tiles = count // block
    cache = jax.ShapeDtypeStruct((WINDOW * PEERS, dim), jnp.bfloat16)
    any_spec = pl.BlockSpec(memory_space=pltpu.HBM)
    args = [me, row_len, new, *own, *pieces]
    in_specs = [pl.BlockSpec(memory_space=pltpu.SMEM)] * 2 + [pl.BlockSpec(memory_space=pltpu.VMEM)] + [any_spec] * (len(own) + len(pieces))
    aliases = {}
    if caches is not None:
        aliases = {len(args): 0, len(args) + 1: 1}
        args += caches
        in_specs += [any_spec] * 2
    return pl.pallas_call(
        functools.partial(interleave_kernel, first, count, block, len(own) == 2, len(aliases)),
        out_shape=[cache, cache],
        in_specs=in_specs,
        out_specs=[any_spec] * 2,
        input_output_aliases=aliases,
        scratch_shapes=[
            pltpu.VMEM((tiles, 2, PEERS, block, dim), jnp.bfloat16),
            pltpu.VMEM((tiles, 2, block * PEERS, dim), jnp.bfloat16),
            pltpu.SemaphoreType.DMA((tiles, 2, PEERS)),
            pltpu.SemaphoreType.DMA((tiles, 2)),
        ],
        compiler_params=pltpu.CompilerParams(vmem_limit_bytes=VMEM_LIMIT),
        cost_estimate=pl.CostEstimate(flops=count * 64 * dim, bytes_accessed=count * PEERS * dim * 8, transcendentals=0),
    )(*args)


def solution(mesh):
    head_spec = P('dp', None, 'sh', None)
    row_spec = P(('dp', 'sh'))
    full_spec = P(None, None)

    def swap(value, offset):
        return lax.ppermute(value, 'sh', [(i, i ^ offset) for i in range(PEERS)])

    def exchange(table, me):
        got = [lax.dynamic_slice_in_dim(table, me ^ offset, 1) for offset in range(PEERS)]
        return [got[0]] + [swap(got[offset], offset) for offset in range(1, PEERS)]

    def by_device(got, me):
        return jnp.take(jnp.concatenate(got, axis=0), me ^ jnp.arange(PEERS), axis=0)

    def per_device(k_prefill, v_prefill, lengths, residual, norm_gain, w_query, w_key, w_value, w_out):
        me = lax.axis_index('sh')
        me_vec = me.reshape(1).astype(jnp.int32)
        seq_len = k_prefill.shape[1]
        head_dim = k_prefill.shape[3]
        k_mine = k_prefill.reshape(PEERS, seq_len, head_dim)
        v_mine = v_prefill.reshape(PEERS, seq_len, head_dim)
        my_len = lax.dynamic_slice_in_dim(lengths, me, 1)
        received = {}

        def send(first, pieces):
            received[first] = [swap(piece, offset) for piece, offset in zip(pieces, ORDER)]

        def start(chunk, after=None, before=None):
            place = me_vec
            if after is not None:
                place, after = lax.optimization_barrier((place, after))
            pieces = pack(*chunk, place, k_mine, v_mine)
            pieces, before = lax.optimization_barrier((pieces, before))
            send(chunk[0], pieces)
            return after, before

        _, residual = start(CHUNKS[0], before=residual)
        _, residual = start(CHUNKS[1], after=residual, before=residual)

        resid_f32 = residual.astype(jnp.float32)
        inv_rms = lax.rsqrt(jnp.mean(resid_f32 * resid_f32, axis=-1, keepdims=True) + EPS)
        normed = (resid_f32 * inv_rms * norm_gain.astype(jnp.float32)).astype(jnp.bfloat16)
        q_heads = jnp.dot(normed, w_query, preferred_element_type=jnp.float32).astype(jnp.bfloat16).reshape(1, -1, head_dim)
        k_new = jnp.dot(normed, w_key, preferred_element_type=jnp.float32).astype(jnp.bfloat16).reshape(1, PEERS, head_dim)
        v_new = jnp.dot(normed, w_value, preferred_element_type=jnp.float32).astype(jnp.bfloat16).reshape(1, PEERS, head_dim)
        q_heads = rotate(q_heads, my_len)
        k_new = rotate(k_new, my_len)
        q_group = q_heads.shape[1] // PEERS
        new = jnp.concatenate([k_new, v_new], axis=0).astype(jnp.float32)

        table = jnp.concatenate([q_heads.reshape(PEERS, q_group, head_dim), k_new.reshape(PEERS, 1, head_dim), v_new.reshape(PEERS, 1, head_dim)], axis=1).reshape(PEERS, -1)
        qkv_parts = exchange(table, me)
        _, table = start(CHUNKS[2], after=table, before=table)
        wrap_place, _ = lax.optimization_barrier((me_vec, table))
        wrapped = wrap_pack(wrap_place, lengths, k_mine, v_mine)
        send(0, wrapped[:-1])
        qkv = by_device(qkv_parts, me).reshape(PEERS, q_group + 2, head_dim)
        q_all, k_all, v_all = qkv[:, :q_group], qkv[:, q_group:q_group + 1], qkv[:, q_group + 1:]
        positions = jnp.arange(seq_len, dtype=jnp.int32)[None, :]
        live = (positions < lengths[:, None]) & (positions > lengths[:, None] - WINDOW)
        scores = jnp.einsum('bgd,bsd->bgs', q_all, k_mine, preferred_element_type=jnp.float32) / head_dim ** 0.5
        scores = jnp.where(live[:, None, :], scores, -jnp.inf)
        top_old = jnp.max(scores, axis=-1, keepdims=True)
        new_score = jnp.sum(q_all.astype(jnp.float32) * k_all.astype(jnp.float32), axis=-1, keepdims=True) / head_dim ** 0.5
        top = jnp.maximum(top_old, new_score)
        exp_scores = jnp.exp(scores - top)
        exp_new = jnp.exp(new_score - top)
        total = jnp.sum(exp_scores, axis=-1, keepdims=True) + exp_new
        weights = (exp_scores / total).astype(jnp.bfloat16)
        new_weight = lax.reduce_precision(exp_new / total, 8, 7)
        mixed = jnp.einsum('bgs,bsd->bgd', weights, v_mine, preferred_element_type=jnp.float32)
        mixed = (mixed + new_weight * v_all.astype(jnp.float32)).astype(jnp.bfloat16).reshape(PEERS, -1)
        attn_parts = exchange(mixed, me)

        place, _ = lax.optimization_barrier((me_vec, mixed))
        caches = None

        def store(first, caches):
            own = [wrapped[-1]] if first == 0 else [k_mine, v_mine]
            return interleave(first, place, my_len, new, own, received[first], caches)

        caches = store(CHUNKS[0][0], caches)
        caches = store(CHUNKS[1][0], caches)
        caches, caches = start(CHUNKS[3], after=caches, before=caches)
        caches, caches = start(CHUNKS[4], after=caches, before=caches)
        caches = store(CHUNKS[2][0], caches)
        attn_parts, caches = lax.optimization_barrier((attn_parts, caches))
        attn_out = by_device(attn_parts, me).reshape(1, -1)
        resid_out = (resid_f32 + jnp.dot(attn_out, w_out, preferred_element_type=jnp.float32)).astype(jnp.bfloat16)
        for first in (0, CHUNKS[3][0], CHUNKS[4][0]):
            caches = store(first, caches)
        shape = (1, WINDOW, PEERS, head_dim)
        return resid_out, caches[0].reshape(shape), caches[1].reshape(shape)

    return jax.shard_map(per_device, mesh=mesh, in_specs=(head_spec, head_spec, P('dp'), P(('dp', 'sh'), None), P(None), full_spec, full_spec, full_spec, full_spec), out_specs=(P(('dp', 'sh'), None), row_spec, row_spec), check_vma=False)
```

```python
import functools

import jax
import jax.numpy as jnp
from jax import lax
from jax.experimental import pallas as pl
from jax.experimental.pallas import tpu as pltpu
from jax.sharding import PartitionSpec as P


WINDOW = 4096
THETA = 10000.0
EPS = 1e-5
PEERS = 8
GROUP = 32
WRAP = 256
CHUNKS = ((256, 256), (512, 1280), (1792, 1280), (3072, 896), (3968, 128))
BLOCK = 256
ORDER = (4, 2, 6, 5, 3, 7, 1)
VMEM_LIMIT = 60 * 1024 * 1024


def rotate(heads, positions):
    head_dim = heads.shape[-1]
    half_dim = head_dim // 2
    inv_freq = THETA ** (-2.0 * jnp.arange(half_dim, dtype=jnp.float32) / head_dim)
    angles = positions.astype(jnp.float32).reshape(positions.shape + (1,) * (heads.ndim - 1)) * inv_freq
    cos_part = jnp.cos(angles)
    sin_part = jnp.sin(angles)
    first_half = heads[..., :half_dim].astype(jnp.float32)
    second_half = heads[..., half_dim:].astype(jnp.float32)
    return jnp.concatenate([first_half * cos_part - second_half * sin_part, second_half * cos_part + first_half * sin_part], axis=-1).astype(jnp.bfloat16)


def pack_kernel(first, count, me_ref, k_ref, v_ref, *refs):
    outs = refs[:len(ORDER)]
    held, in_sems, out_sems = refs[len(ORDER):]
    me = me_ref[0]
    reads = []
    for at, offset in enumerate(ORDER):
        for kv, src in enumerate((k_ref, v_ref)):
            reads.append(pltpu.make_async_copy(src.at[me ^ offset, pl.ds(first, count)], held.at[at, kv], in_sems.at[at, kv]))
            reads[-1].start()
    writes = []
    for at, out in enumerate(outs):
        reads[2 * at].wait()
        reads[2 * at + 1].wait()
        writes.append(pltpu.make_async_copy(held.at[at], out, out_sems.at[at]))
        writes[-1].start()
    for write in writes:
        write.wait()


def pack(first, count, me, k_mine, v_mine):
    dim = k_mine.shape[2]
    piece = jax.ShapeDtypeStruct((2, count, dim), jnp.bfloat16)
    return pl.pallas_call(
        functools.partial(pack_kernel, first, count),
        out_shape=[piece] * len(ORDER),
        in_specs=[pl.BlockSpec(memory_space=pltpu.SMEM)] + [pl.BlockSpec(memory_space=pltpu.HBM)] * 2,
        out_specs=[pl.BlockSpec(memory_space=pltpu.HBM)] * len(ORDER),
        scratch_shapes=[pltpu.VMEM((len(ORDER), 2, count, dim), jnp.bfloat16), pltpu.SemaphoreType.DMA((len(ORDER), 2)), pltpu.SemaphoreType.DMA((len(ORDER),))],
        compiler_params=pltpu.CompilerParams(vmem_limit_bytes=VMEM_LIMIT),
        cost_estimate=pl.CostEstimate(flops=0, bytes_accessed=len(ORDER) * 4 * count * dim * 2, transcendentals=0),
    )(me, k_mine, v_mine)


def wrap_kernel(me_ref, len_ref, k_ref, k_late_ref, v_ref, v_late_ref, *outs):
    me = me_ref[0]
    slots = lax.broadcasted_iota(jnp.int32, (WRAP, 128), 0)
    for out, offset in zip(outs, ORDER + (0,)):
        row = me ^ offset
        late = slots + WINDOW < len_ref[row]
        for kv, (base_ref, late_ref) in enumerate(((k_ref, k_late_ref), (v_ref, v_late_ref))):
            out[kv] = jnp.where(late, late_ref[row].astype(jnp.float32), base_ref[row].astype(jnp.float32)).astype(jnp.bfloat16)


def wrap_pack(me, lengths, k_mine, v_mine):
    rows, _, dim = k_mine.shape
    base = pl.BlockSpec((rows, WRAP, dim), lambda i: (0, 0, 0))
    late = pl.BlockSpec((rows, WRAP, dim), lambda i: (0, WINDOW // WRAP, 0))
    piece = jax.ShapeDtypeStruct((2, WRAP, dim), jnp.bfloat16)
    return pl.pallas_call(
        wrap_kernel,
        grid=(1,),
        out_shape=[piece] * (len(ORDER) + 1),
        out_specs=[pl.BlockSpec((2, WRAP, dim), lambda i: (0, 0, 0))] * (len(ORDER) + 1),
        in_specs=[pl.BlockSpec(memory_space=pltpu.SMEM)] * 2 + [base, late, base, late],
        compiler_params=pltpu.CompilerParams(vmem_limit_bytes=VMEM_LIMIT),
        cost_estimate=pl.CostEstimate(flops=rows * 8 * WRAP * dim, bytes_accessed=rows * 6 * WRAP * dim * 2, transcendentals=0),
    )(me, lengths, k_mine, k_mine, v_mine, v_mine)


def interleave_kernel(first, count, block, has_own, num_alias, me_ref, len_ref, new_ref, *refs):
    num_own = 2 if has_own else 1
    own = refs[:num_own]
    pieces = refs[num_own:num_own + len(ORDER)]
    k_out, v_out, held, mixed, in_sems, out_sems = refs[num_own + len(ORDER) + num_alias:]
    tiles = count // block
    me = me_ref[0]
    row_len = len_ref[0]
    new_slot = lax.rem(row_len, WINDOW)
    outs = (k_out, v_out)

    def read(tile, kv, offset):
        at = pl.multiple_of(tile * block, block)
        if offset:
            src = pieces[ORDER.index(offset)].at[kv, pl.ds(at, block)]
        elif has_own:
            src = own[kv].at[me, pl.ds(first + at, block)]
        else:
            src = own[0].at[kv, pl.ds(at, block)]
        return pltpu.make_async_copy(src, held.at[tile, kv, me ^ offset], in_sems.at[tile, kv, offset])

    def write(tile, kv):
        at = pl.multiple_of((first + tile * block) * PEERS, block * PEERS)
        return pltpu.make_async_copy(mixed.at[tile, kv], outs[kv].at[pl.ds(at, block * PEERS)], out_sems.at[tile, kv])

    @pl.loop(0, tiles)
    def _(tile):
        for kv in range(2):
            for offset in range(PEERS):
                read(tile, kv, offset).start()

    @pl.loop(0, tiles)
    def _(tile):
        start = first + tile * block
        plain = (start + block <= row_len) & ((new_slot < start) | (new_slot >= start + block))
        for kv in range(2):
            for offset in range(PEERS):
                read(tile, kv, offset).wait()

            def group(at):
                return jnp.swapaxes(held[tile, kv, :, at:at + GROUP, :], 0, 1).reshape(GROUP * PEERS, -1)

            @pl.when(plain)
            def _():
                for at in range(0, block, GROUP):
                    mixed[tile, kv, at * PEERS:(at + GROUP) * PEERS, :] = group(at)

            @pl.when(jnp.logical_not(plain))
            def _():
                new = jnp.concatenate([new_ref[kv]] * GROUP, axis=0)
                slot_of_row = lax.broadcasted_iota(jnp.int32, new.shape, 0) // PEERS
                for at in range(0, block, GROUP):
                    slots = slot_of_row + (start + at)
                    rows = jnp.where(slots < row_len, group(at).astype(jnp.float32), 0.0)
                    rows = jnp.where(slots == new_slot, new, rows)
                    mixed[tile, kv, at * PEERS:(at + GROUP) * PEERS, :] = rows.astype(jnp.bfloat16)

            write(tile, kv).start()

    @pl.loop(0, tiles)
    def _(tile):
        for kv in range(2):
            write(tile, kv).wait()


def interleave(first, me, row_len, new, own, pieces, caches):
    count, dim = pieces[0].shape[1:]
    block = BLOCK if count % BLOCK == 0 else BLOCK // 2
    tiles = count // block
    cache = jax.ShapeDtypeStruct((WINDOW * PEERS, dim), jnp.bfloat16)
    any_spec = pl.BlockSpec(memory_space=pltpu.HBM)
    args = [me, row_len, new, *own, *pieces]
    in_specs = [pl.BlockSpec(memory_space=pltpu.SMEM)] * 2 + [pl.BlockSpec(memory_space=pltpu.VMEM)] + [any_spec] * (len(own) + len(pieces))
    aliases = {}
    if caches is not None:
        aliases = {len(args): 0, len(args) + 1: 1}
        args += caches
        in_specs += [any_spec] * 2
    return pl.pallas_call(
        functools.partial(interleave_kernel, first, count, block, len(own) == 2, len(aliases)),
        out_shape=[cache, cache],
        in_specs=in_specs,
        out_specs=[any_spec] * 2,
        input_output_aliases=aliases,
        scratch_shapes=[
            pltpu.VMEM((tiles, 2, PEERS, block, dim), jnp.bfloat16),
            pltpu.VMEM((tiles, 2, block * PEERS, dim), jnp.bfloat16),
            pltpu.SemaphoreType.DMA((tiles, 2, PEERS)),
            pltpu.SemaphoreType.DMA((tiles, 2)),
        ],
        compiler_params=pltpu.CompilerParams(vmem_limit_bytes=VMEM_LIMIT),
        cost_estimate=pl.CostEstimate(flops=count * 64 * dim, bytes_accessed=count * PEERS * dim * 8, transcendentals=0),
    )(*args)


def solution(mesh):
    head_spec = P('dp', None, 'sh', None)
    row_spec = P(('dp', 'sh'))
    full_spec = P(None, None)

    def swap(value, offset):
        return lax.ppermute(value, 'sh', [(i, i ^ offset) for i in range(PEERS)])

    def exchange(table, me):
        got = [lax.dynamic_slice_in_dim(table, me ^ offset, 1) for offset in range(PEERS)]
        return [got[0]] + [swap(got[offset], offset) for offset in range(1, PEERS)]

    def by_device(got, me):
        return jnp.take(jnp.concatenate(got, axis=0), me ^ jnp.arange(PEERS), axis=0)

    def per_device(k_prefill, v_prefill, lengths, residual, norm_gain, w_query, w_key, w_value, w_out):
        me = lax.axis_index('sh')
        me_vec = me.reshape(1).astype(jnp.int32)
        seq_len = k_prefill.shape[1]
        head_dim = k_prefill.shape[3]
        k_mine = k_prefill.reshape(PEERS, seq_len, head_dim)
        v_mine = v_prefill.reshape(PEERS, seq_len, head_dim)
        my_len = lax.dynamic_slice_in_dim(lengths, me, 1)
        received = {}

        def send(first, pieces):
            received[first] = [swap(piece, offset) for piece, offset in zip(pieces, ORDER)]

        def start(chunk, after=None, before=None):
            place = me_vec
            if after is not None:
                place, after = lax.optimization_barrier((place, after))
            pieces = pack(*chunk, place, k_mine, v_mine)
            pieces, before = lax.optimization_barrier((pieces, before))
            send(chunk[0], pieces)
            return after, before

        _, residual = start(CHUNKS[0], before=residual)
        _, residual = start(CHUNKS[1], after=residual, before=residual)

        resid_f32 = residual.astype(jnp.float32)
        inv_rms = lax.rsqrt(jnp.mean(resid_f32 * resid_f32, axis=-1, keepdims=True) + EPS)
        normed = (resid_f32 * inv_rms * norm_gain.astype(jnp.float32)).astype(jnp.bfloat16)
        q_heads = jnp.dot(normed, w_query, preferred_element_type=jnp.float32).astype(jnp.bfloat16).reshape(1, -1, head_dim)
        k_new = jnp.dot(normed, w_key, preferred_element_type=jnp.float32).astype(jnp.bfloat16).reshape(1, PEERS, head_dim)
        v_new = jnp.dot(normed, w_value, preferred_element_type=jnp.float32).astype(jnp.bfloat16).reshape(1, PEERS, head_dim)
        q_heads = rotate(q_heads, my_len)
        k_new = rotate(k_new, my_len)
        q_group = q_heads.shape[1] // PEERS
        new = jnp.concatenate([k_new, v_new], axis=0).astype(jnp.float32)

        table = jnp.concatenate([q_heads.reshape(PEERS, q_group, head_dim), k_new.reshape(PEERS, 1, head_dim), v_new.reshape(PEERS, 1, head_dim)], axis=1).reshape(PEERS, -1)
        qkv_parts = exchange(table, me)
        _, table = start(CHUNKS[2], after=table, before=table)
        wrap_place, _ = lax.optimization_barrier((me_vec, table))
        wrapped = wrap_pack(wrap_place, lengths, k_mine, v_mine)
        send(0, wrapped[:-1])
        qkv = by_device(qkv_parts, me).reshape(PEERS, q_group + 2, head_dim)
        q_all, k_all, v_all = qkv[:, :q_group], qkv[:, q_group:q_group + 1], qkv[:, q_group + 1:]
        positions = jnp.arange(seq_len, dtype=jnp.int32)[None, :]
        live = (positions < lengths[:, None]) & (positions > lengths[:, None] - WINDOW)
        scores = jnp.einsum('bgd,bsd->bgs', q_all, k_mine, preferred_element_type=jnp.float32) / head_dim ** 0.5
        scores = jnp.where(live[:, None, :], scores, -jnp.inf)
        top_old = jnp.max(scores, axis=-1, keepdims=True)
        new_score = jnp.sum(q_all.astype(jnp.float32) * k_all.astype(jnp.float32), axis=-1, keepdims=True) / head_dim ** 0.5
        top = jnp.maximum(top_old, new_score)
        exp_scores = jnp.exp(scores - top)
        exp_new = jnp.exp(new_score - top)
        total = jnp.sum(exp_scores, axis=-1, keepdims=True) + exp_new
        weights = (exp_scores / total).astype(jnp.bfloat16)
        new_weight = lax.reduce_precision(exp_new / total, 8, 7)
        mixed = jnp.einsum('bgs,bsd->bgd', weights, v_mine, preferred_element_type=jnp.float32)
        mixed = (mixed + new_weight * v_all.astype(jnp.float32)).astype(jnp.bfloat16).reshape(PEERS, -1)
        attn_parts = exchange(mixed, me)

        place, _ = lax.optimization_barrier((me_vec, mixed))
        caches = None

        def store(first, caches):
            own = [wrapped[-1]] if first == 0 else [k_mine, v_mine]
            return interleave(first, place, my_len, new, own, received[first], caches)

        caches = store(CHUNKS[0][0], caches)
        caches = store(CHUNKS[1][0], caches)
        caches, caches = start(CHUNKS[3], after=caches, before=caches)
        caches, caches = start(CHUNKS[4], after=caches, before=caches)
        caches = store(CHUNKS[2][0], caches)
        attn_parts, caches = lax.optimization_barrier((attn_parts, caches))
        attn_out = by_device(attn_parts, me).reshape(1, -1)
        resid_out = (resid_f32 + jnp.dot(attn_out, w_out, preferred_element_type=jnp.float32)).astype(jnp.bfloat16)
        for first in (0, CHUNKS[3][0], CHUNKS[4][0]):
            caches = store(first, caches)
        shape = (1, WINDOW, PEERS, head_dim)
        return resid_out, caches[0].reshape(shape), caches[1].reshape(shape)

    return jax.shard_map(per_device, mesh=mesh, in_specs=(head_spec, head_spec, P('dp'), P(('dp', 'sh'), None), P(None), full_spec, full_spec, full_spec, full_spec), out_specs=(P(('dp', 'sh'), None), row_spec, row_spec), check_vma=False)
```

```python
import functools

import jax
import jax.numpy as jnp
from jax import lax
from jax.experimental import pallas as pl
from jax.experimental.pallas import tpu as pltpu
from jax.sharding import PartitionSpec as P


WINDOW = 4096
THETA = 10000.0
EPS = 1e-5
PEERS = 8
GROUP = 32
WRAP = 256
CHUNKS = ((256, 256), (512, 1280), (1792, 1280), (3072, 640), (3712, 256), (3968, 128))
BLOCK = 256
ORDER = (6, 4, 2, 7, 5, 3, 1)
VMEM_LIMIT = 56 * 1024 * 1024
LAST_VMEM_LIMIT = 8 * 1024 * 1024


def rotate(heads, positions):
    head_dim = heads.shape[-1]
    half_dim = head_dim // 2
    inv_freq = THETA ** (-2.0 * jnp.arange(half_dim, dtype=jnp.float32) / head_dim)
    angles = positions.astype(jnp.float32).reshape(positions.shape + (1,) * (heads.ndim - 1)) * inv_freq
    cos_part = jnp.cos(angles)
    sin_part = jnp.sin(angles)
    first_half = heads[..., :half_dim].astype(jnp.float32)
    second_half = heads[..., half_dim:].astype(jnp.float32)
    return jnp.concatenate([first_half * cos_part - second_half * sin_part, second_half * cos_part + first_half * sin_part], axis=-1).astype(jnp.bfloat16)


def pack_kernel(first, count, has_own, me_ref, k_ref, v_ref, *refs):
    offsets = ORDER + (0,) * has_own
    outs, sems = refs[:-1], refs[-1]
    me = me_ref[0]
    copies = []
    for at, offset in enumerate(offsets):
        for kv, src in enumerate((k_ref, v_ref)):
            copies.append(pltpu.make_async_copy(src.at[me ^ offset, pl.ds(first, count)], outs[at].at[kv], sems.at[at, kv]))
            copies[-1].start()
    for copy in copies:
        copy.wait()


def pack(first, count, has_own, me, k_mine, v_mine):
    dim = k_mine.shape[2]
    pieces = len(ORDER) + has_own
    return pl.pallas_call(
        functools.partial(pack_kernel, first, count, has_own),
        out_shape=[jax.ShapeDtypeStruct((2, count, dim), jnp.bfloat16)] * pieces,
        in_specs=[pl.BlockSpec(memory_space=pltpu.SMEM)] + [pl.BlockSpec(memory_space=pltpu.HBM)] * 2,
        out_specs=[pl.BlockSpec(memory_space=pltpu.VMEM)] * pieces,
        scratch_shapes=[pltpu.SemaphoreType.DMA((pieces, 2))],
        compiler_params=pltpu.CompilerParams(vmem_limit_bytes=VMEM_LIMIT),
        cost_estimate=pl.CostEstimate(flops=0, bytes_accessed=pieces * 4 * count * dim * 2, transcendentals=0),
    )(me, k_mine, v_mine)


def wrap_kernel(me_ref, len_ref, k_ref, k_late_ref, v_ref, v_late_ref, *outs):
    me = me_ref[0]
    slots = lax.broadcasted_iota(jnp.int32, (WRAP, 128), 0)
    for out, offset in zip(outs, ORDER + (0,)):
        row = me ^ offset
        late = slots + WINDOW < len_ref[row]
        for kv, (base_ref, late_ref) in enumerate(((k_ref, k_late_ref), (v_ref, v_late_ref))):
            out[kv] = jnp.where(late, late_ref[row].astype(jnp.float32), base_ref[row].astype(jnp.float32)).astype(jnp.bfloat16)


def wrap_pack(me, lengths, k_mine, v_mine):
    rows, _, dim = k_mine.shape
    base = pl.BlockSpec((rows, WRAP, dim), lambda i: (0, 0, 0))
    late = pl.BlockSpec((rows, WRAP, dim), lambda i: (0, WINDOW // WRAP, 0))
    piece = jax.ShapeDtypeStruct((2, WRAP, dim), jnp.bfloat16)
    return pl.pallas_call(
        wrap_kernel,
        grid=(1,),
        out_shape=[piece] * (len(ORDER) + 1),
        out_specs=[pl.BlockSpec((2, WRAP, dim), lambda i: (0, 0, 0))] * (len(ORDER) + 1),
        in_specs=[pl.BlockSpec(memory_space=pltpu.SMEM)] * 2 + [base, late, base, late],
        compiler_params=pltpu.CompilerParams(vmem_limit_bytes=VMEM_LIMIT),
        cost_estimate=pl.CostEstimate(flops=rows * 8 * WRAP * dim, bytes_accessed=rows * 6 * WRAP * dim * 2, transcendentals=0),
    )(me, lengths, k_mine, k_mine, v_mine, v_mine)


def interleave_kernel(first, count, block, has_own, num_alias, me_ref, len_ref, new_ref, *refs):
    num_own = 2 if has_own else 1
    own = refs[:num_own]
    pieces = refs[num_own:num_own + len(ORDER)]
    k_out, v_out, held, mixed, in_sems, out_sems = refs[num_own + len(ORDER) + num_alias:]
    tiles = count // block
    me = me_ref[0]
    row_len = len_ref[0]
    new_slot = lax.rem(row_len, WINDOW)
    outs = (k_out, v_out)

    def read(tile, kv, offset):
        at = pl.multiple_of(tile * block, block)
        if offset:
            src = pieces[ORDER.index(offset)].at[kv, pl.ds(at, block)]
        elif has_own:
            src = own[kv].at[me, pl.ds(first + at, block)]
        else:
            src = own[0].at[kv, pl.ds(at, block)]
        return pltpu.make_async_copy(src, held.at[tile, kv, me ^ offset], in_sems.at[tile, kv, offset])

    def write(tile, kv):
        at = pl.multiple_of((first + tile * block) * PEERS, block * PEERS)
        return pltpu.make_async_copy(mixed.at[tile, kv], outs[kv].at[pl.ds(at, block * PEERS)], out_sems.at[tile, kv])

    @pl.loop(0, tiles)
    def _(tile):
        for kv in range(2):
            for offset in range(PEERS):
                read(tile, kv, offset).start()

    @pl.loop(0, tiles)
    def _(tile):
        start = first + tile * block
        plain = (start + block <= row_len) & ((new_slot < start) | (new_slot >= start + block))
        for kv in range(2):
            for offset in range(PEERS):
                read(tile, kv, offset).wait()

            def group(at):
                return jnp.swapaxes(held[tile, kv, :, at:at + GROUP, :], 0, 1).reshape(GROUP * PEERS, -1)

            @pl.when(plain)
            def _():
                for at in range(0, block, GROUP):
                    mixed[tile, kv, at * PEERS:(at + GROUP) * PEERS, :] = group(at)

            @pl.when(jnp.logical_not(plain))
            def _():
                new = jnp.concatenate([new_ref[kv]] * GROUP, axis=0)
                slot_of_row = lax.broadcasted_iota(jnp.int32, new.shape, 0) // PEERS
                for at in range(0, block, GROUP):
                    slots = slot_of_row + (start + at)
                    rows = jnp.where(slots < row_len, group(at).astype(jnp.float32), 0.0)
                    rows = jnp.where(slots == new_slot, new, rows)
                    mixed[tile, kv, at * PEERS:(at + GROUP) * PEERS, :] = rows.astype(jnp.bfloat16)

            write(tile, kv).start()

    @pl.loop(0, tiles)
    def _(tile):
        for kv in range(2):
            write(tile, kv).wait()


def interleave(first, me, row_len, new, own, pieces, caches):
    count, dim = pieces[0].shape[1:]
    block = BLOCK if count % BLOCK == 0 else BLOCK // 2
    tiles = count // block
    cache = jax.ShapeDtypeStruct((WINDOW * PEERS, dim), jnp.bfloat16)
    any_spec = pl.BlockSpec(memory_space=pltpu.HBM)
    args = [me, row_len, new, *own, *pieces]
    in_specs = [pl.BlockSpec(memory_space=pltpu.SMEM)] * 2 + [pl.BlockSpec(memory_space=pltpu.VMEM)] + [any_spec] * (len(own) + len(pieces))
    aliases = {}
    if caches is not None:
        aliases = {len(args): 0, len(args) + 1: 1}
        args += caches
        in_specs += [any_spec] * 2
    return pl.pallas_call(
        functools.partial(interleave_kernel, first, count, block, len(own) == 2, len(aliases)),
        out_shape=[cache, cache],
        in_specs=in_specs,
        out_specs=[any_spec] * 2,
        input_output_aliases=aliases,
        scratch_shapes=[
            pltpu.VMEM((tiles, 2, PEERS, block, dim), jnp.bfloat16),
            pltpu.VMEM((tiles, 2, block * PEERS, dim), jnp.bfloat16),
            pltpu.SemaphoreType.DMA((tiles, 2, PEERS)),
            pltpu.SemaphoreType.DMA((tiles, 2)),
        ],
        compiler_params=pltpu.CompilerParams(vmem_limit_bytes=VMEM_LIMIT),
        cost_estimate=pl.CostEstimate(flops=count * 64 * dim, bytes_accessed=count * PEERS * dim * 8, transcendentals=0),
    )(*args)


def last_kernel(first, count, me_ref, len_ref, new_ref, *refs):
    pieces = refs[:PEERS]
    k_out, v_out, mixed, sems = refs[PEERS + 2:]
    me = me_ref[0]
    row_len = len_ref[0]
    new_slot = lax.rem(row_len, WINDOW)
    by_offset = pieces[-1:] + tuple(pieces[ORDER.index(offset)] for offset in range(1, PEERS))
    copies = []
    for kv, out in enumerate((k_out, v_out)):
        new = jnp.concatenate([new_ref[kv]] * GROUP, axis=0)
        slot_of_row = lax.broadcasted_iota(jnp.int32, new.shape, 0) // PEERS
        for at in range(0, count, GROUP):
            heads = [ref[kv, at:at + GROUP, :] for ref in by_offset]
            for bit in (1, 2, 4):
                swapped = (me & bit) != 0
                heads = [jnp.where(swapped, heads[head ^ bit], heads[head]) for head in range(PEERS)]
            rows = jnp.swapaxes(jnp.stack(heads, axis=0), 0, 1).reshape(GROUP * PEERS, -1)
            slots = slot_of_row + (first + at)
            rows = jnp.where(slots < row_len, rows.astype(jnp.float32), 0.0)
            rows = jnp.where(slots == new_slot, new, rows)
            mixed[kv, at * PEERS:(at + GROUP) * PEERS, :] = rows.astype(jnp.bfloat16)
        copies.append(pltpu.make_async_copy(mixed.at[kv], out.at[pl.ds(first * PEERS, count * PEERS)], sems.at[kv]))
        copies[-1].start()
    for copy in copies:
        copy.wait()


def interleave_last(first, me, row_len, new, pieces, caches):
    count, dim = pieces[0].shape[1:]
    cache = jax.ShapeDtypeStruct((WINDOW * PEERS, dim), jnp.bfloat16)
    return pl.pallas_call(
        functools.partial(last_kernel, first, count),
        out_shape=[cache, cache],
        in_specs=[pl.BlockSpec(memory_space=pltpu.SMEM)] * 2 + [pl.BlockSpec(memory_space=pltpu.VMEM)] * (1 + PEERS) + [pl.BlockSpec(memory_space=pltpu.HBM)] * 2,
        out_specs=[pl.BlockSpec(memory_space=pltpu.HBM)] * 2,
        input_output_aliases={3 + PEERS: 0, 4 + PEERS: 1},
        scratch_shapes=[pltpu.VMEM((2, count * PEERS, dim), jnp.bfloat16), pltpu.SemaphoreType.DMA((2,))],
        compiler_params=pltpu.CompilerParams(vmem_limit_bytes=LAST_VMEM_LIMIT),
        cost_estimate=pl.CostEstimate(flops=count * 64 * dim, bytes_accessed=count * PEERS * dim * 8, transcendentals=0),
    )(me, row_len, new, *pieces, *caches)


def solution(mesh):
    head_spec = P('dp', None, 'sh', None)
    row_spec = P(('dp', 'sh'))
    full_spec = P(None, None)

    def swap(value, offset):
        return lax.ppermute(value, 'sh', [(i, i ^ offset) for i in range(PEERS)])

    def exchange(table, me):
        got = [lax.dynamic_slice_in_dim(table, me ^ offset, 1) for offset in range(PEERS)]
        return [got[0]] + [swap(got[offset], offset) for offset in range(1, PEERS)]

    def by_device(got, me):
        return jnp.take(jnp.concatenate(got, axis=0), me ^ jnp.arange(PEERS), axis=0)

    def per_device(k_prefill, v_prefill, lengths, residual, norm_gain, w_query, w_key, w_value, w_out):
        me = lax.axis_index('sh')
        me_vec = me.reshape(1).astype(jnp.int32)
        seq_len = k_prefill.shape[1]
        head_dim = k_prefill.shape[3]
        k_mine = k_prefill.reshape(PEERS, seq_len, head_dim)
        v_mine = v_prefill.reshape(PEERS, seq_len, head_dim)
        my_len = lax.dynamic_slice_in_dim(lengths, me, 1)
        received = {}

        def send(first, pieces):
            received[first] = [swap(piece, offset) for piece, offset in zip(pieces, ORDER)]

        def start(chunk, after=None, before=None):
            place = me_vec
            if after is not None:
                place, after = lax.optimization_barrier((place, after))
            pieces = pack(*chunk, chunk == CHUNKS[-1], place, k_mine, v_mine)
            pieces, before = lax.optimization_barrier((pieces, before))
            send(chunk[0], pieces)
            received[chunk[0]] += pieces[len(ORDER):]
            return after, before

        _, residual = start(CHUNKS[0], before=residual)
        _, residual = start(CHUNKS[1], after=residual, before=residual)

        resid_f32 = residual.astype(jnp.float32)
        inv_rms = lax.rsqrt(jnp.mean(resid_f32 * resid_f32, axis=-1, keepdims=True) + EPS)
        normed = (resid_f32 * inv_rms * norm_gain.astype(jnp.float32)).astype(jnp.bfloat16)
        q_heads = jnp.dot(normed, w_query, preferred_element_type=jnp.float32).astype(jnp.bfloat16).reshape(1, -1, head_dim)
        k_new = jnp.dot(normed, w_key, preferred_element_type=jnp.float32).astype(jnp.bfloat16).reshape(1, PEERS, head_dim)
        v_new = jnp.dot(normed, w_value, preferred_element_type=jnp.float32).astype(jnp.bfloat16).reshape(1, PEERS, head_dim)
        q_heads = rotate(q_heads, my_len)
        k_new = rotate(k_new, my_len)
        q_group = q_heads.shape[1] // PEERS
        new = jnp.concatenate([k_new, v_new], axis=0).astype(jnp.float32)

        table = jnp.concatenate([q_heads.reshape(PEERS, q_group, head_dim), k_new.reshape(PEERS, 1, head_dim), v_new.reshape(PEERS, 1, head_dim)], axis=1).reshape(PEERS, -1)
        qkv_parts = exchange(table, me)
        _, table = start(CHUNKS[2], after=table, before=table)
        wrap_place, _ = lax.optimization_barrier((me_vec, table))
        wrapped = wrap_pack(wrap_place, lengths, k_mine, v_mine)
        send(0, wrapped[:-1])
        qkv = by_device(qkv_parts, me).reshape(PEERS, q_group + 2, head_dim)
        q_all, k_all, v_all = qkv[:, :q_group], qkv[:, q_group:q_group + 1], qkv[:, q_group + 1:]
        positions = jnp.arange(seq_len, dtype=jnp.int32)[None, :]
        live = (positions < lengths[:, None]) & (positions > lengths[:, None] - WINDOW)
        scores = jnp.einsum('bgd,bsd->bgs', q_all, k_mine, preferred_element_type=jnp.float32) / head_dim ** 0.5
        scores = jnp.where(live[:, None, :], scores, -jnp.inf)
        top_old = jnp.max(scores, axis=-1, keepdims=True)
        new_score = jnp.sum(q_all.astype(jnp.float32) * k_all.astype(jnp.float32), axis=-1, keepdims=True) / head_dim ** 0.5
        top = jnp.maximum(top_old, new_score)
        exp_scores = jnp.exp(scores - top)
        exp_new = jnp.exp(new_score - top)
        total = jnp.sum(exp_scores, axis=-1, keepdims=True) + exp_new
        weights = (exp_scores / total).astype(jnp.bfloat16)
        new_weight = lax.reduce_precision(exp_new / total, 8, 7)
        mixed = jnp.einsum('bgs,bsd->bgd', weights, v_mine, preferred_element_type=jnp.float32)
        mixed = (mixed + new_weight * v_all.astype(jnp.float32)).astype(jnp.bfloat16).reshape(PEERS, -1)
        attn_parts = exchange(mixed, me)

        place, _ = lax.optimization_barrier((me_vec, mixed))
        caches = None

        def store(first, caches):
            own = [wrapped[-1]] if first == 0 else [k_mine, v_mine]
            if first == CHUNKS[-1][0]:
                return interleave_last(first, place, my_len, new, received[first], caches)
            return interleave(first, place, my_len, new, own, received[first], caches)

        caches = store(CHUNKS[0][0], caches)
        caches = store(CHUNKS[1][0], caches)
        caches, caches = start(CHUNKS[3], after=caches, before=caches)
        caches, caches = start(CHUNKS[4], after=caches, before=caches)
        caches = store(CHUNKS[2][0], caches)
        caches, caches = start(CHUNKS[5], after=caches, before=caches)
        attn_parts, caches = lax.optimization_barrier((attn_parts, caches))
        attn_out = by_device(attn_parts, me).reshape(1, -1)
        resid_out = (resid_f32 + jnp.dot(attn_out, w_out, preferred_element_type=jnp.float32)).astype(jnp.bfloat16)
        for first in (0,) + tuple(chunk[0] for chunk in CHUNKS[3:]):
            caches = store(first, caches)
        shape = (1, WINDOW, PEERS, head_dim)
        return resid_out, caches[0].reshape(shape), caches[1].reshape(shape)

    return jax.shard_map(per_device, mesh=mesh, in_specs=(head_spec, head_spec, P('dp'), P(('dp', 'sh'), None), P(None), full_spec, full_spec, full_spec, full_spec), out_specs=(P(('dp', 'sh'), None), row_spec, row_spec), check_vma=False)
```

```python
import functools

import jax
import jax.numpy as jnp
from jax import lax
from jax.experimental import pallas as pl
from jax.experimental.pallas import tpu as pltpu
from jax.sharding import PartitionSpec as P


WINDOW = 4096
THETA = 10000.0
EPS = 1e-5
PEERS = 8
GROUP = 32
WRAP = 256
CHUNKS = ((256, 256), (512, 1280), (1792, 1280), (3072, 640), (3712, 256), (3968, 128))
BLOCK = 256
ORDER = (6, 4, 2, 7, 5, 3, 1)
VMEM_LIMIT = 56 * 1024 * 1024
LAST_VMEM_LIMIT = 8 * 1024 * 1024


def rotate(heads, positions):
    head_dim = heads.shape[-1]
    half_dim = head_dim // 2
    inv_freq = THETA ** (-2.0 * jnp.arange(half_dim, dtype=jnp.float32) / head_dim)
    angles = positions.astype(jnp.float32).reshape(positions.shape + (1,) * (heads.ndim - 1)) * inv_freq
    cos_part = jnp.cos(angles)
    sin_part = jnp.sin(angles)
    first_half = heads[..., :half_dim].astype(jnp.float32)
    second_half = heads[..., half_dim:].astype(jnp.float32)
    return jnp.concatenate([first_half * cos_part - second_half * sin_part, second_half * cos_part + first_half * sin_part], axis=-1).astype(jnp.bfloat16)


def pack_kernel(first, count, has_own, k_ref, v_ref, *refs):
    offsets = ORDER + (0,) * has_own
    outs, sems = refs[:-1], refs[-1]
    me = lax.axis_index('sh')
    copies = []
    for at, offset in enumerate(offsets):
        for kv, src in enumerate((k_ref, v_ref)):
            copies.append(pltpu.make_async_copy(src.at[me ^ offset, pl.ds(first, count)], outs[at].at[kv], sems.at[at, kv]))
            copies[-1].start()
    for copy in copies:
        copy.wait()


def pack(first, count, has_own, k_mine, v_mine):
    dim = k_mine.shape[2]
    pieces = len(ORDER) + has_own
    return pl.pallas_call(
        functools.partial(pack_kernel, first, count, has_own),
        out_shape=[jax.ShapeDtypeStruct((2, count, dim), jnp.bfloat16)] * pieces,
        in_specs=[pl.BlockSpec(memory_space=pltpu.HBM)] * 2,
        out_specs=[pl.BlockSpec(memory_space=pltpu.VMEM)] * pieces,
        scratch_shapes=[pltpu.SemaphoreType.DMA((pieces, 2))],
        compiler_params=pltpu.CompilerParams(vmem_limit_bytes=VMEM_LIMIT),
        cost_estimate=pl.CostEstimate(flops=0, bytes_accessed=pieces * 4 * count * dim * 2, transcendentals=0),
    )(k_mine, v_mine)


def wrap_kernel(len_ref, k_ref, k_late_ref, v_ref, v_late_ref, *outs):
    me = lax.axis_index('sh')
    slots = lax.broadcasted_iota(jnp.int32, (WRAP, 128), 0)
    for out, offset in zip(outs, ORDER + (0,)):
        row = me ^ offset
        late = slots + WINDOW < len_ref[row]
        for kv, (base_ref, late_ref) in enumerate(((k_ref, k_late_ref), (v_ref, v_late_ref))):
            out[kv] = jnp.where(late, late_ref[row].astype(jnp.float32), base_ref[row].astype(jnp.float32)).astype(jnp.bfloat16)


def wrap_pack(lengths, k_mine, v_mine):
    rows, _, dim = k_mine.shape
    base = pl.BlockSpec((rows, WRAP, dim), lambda i: (0, 0, 0))
    late = pl.BlockSpec((rows, WRAP, dim), lambda i: (0, WINDOW // WRAP, 0))
    piece = jax.ShapeDtypeStruct((2, WRAP, dim), jnp.bfloat16)
    return pl.pallas_call(
        wrap_kernel,
        grid=(1,),
        out_shape=[piece] * (len(ORDER) + 1),
        out_specs=[pl.BlockSpec((2, WRAP, dim), lambda i: (0, 0, 0))] * (len(ORDER) + 1),
        in_specs=[pl.BlockSpec(memory_space=pltpu.SMEM), base, late, base, late],
        compiler_params=pltpu.CompilerParams(vmem_limit_bytes=VMEM_LIMIT),
        cost_estimate=pl.CostEstimate(flops=rows * 8 * WRAP * dim, bytes_accessed=rows * 6 * WRAP * dim * 2, transcendentals=0),
    )(lengths, k_mine, k_mine, v_mine, v_mine)


def interleave_kernel(first, count, block, has_own, num_alias, len_ref, new_ref, *refs):
    num_own = 2 if has_own else 1
    own = refs[:num_own]
    pieces = refs[num_own:num_own + len(ORDER)]
    k_out, v_out, held, mixed, in_sems, out_sems = refs[num_own + len(ORDER) + num_alias:]
    tiles = count // block
    me = lax.axis_index('sh')
    row_len = len_ref[0]
    new_slot = lax.rem(row_len, WINDOW)
    outs = (k_out, v_out)

    def read(tile, kv, offset):
        at = pl.multiple_of(tile * block, block)
        if offset:
            src = pieces[ORDER.index(offset)].at[kv, pl.ds(at, block)]
        elif has_own:
            src = own[kv].at[me, pl.ds(first + at, block)]
        else:
            src = own[0].at[kv, pl.ds(at, block)]
        return pltpu.make_async_copy(src, held.at[tile, kv, me ^ offset], in_sems.at[tile, kv, offset])

    def write(tile, kv):
        at = pl.multiple_of((first + tile * block) * PEERS, block * PEERS)
        return pltpu.make_async_copy(mixed.at[tile, kv], outs[kv].at[pl.ds(at, block * PEERS)], out_sems.at[tile, kv])

    @pl.loop(0, tiles)
    def _(tile):
        for kv in range(2):
            for offset in range(PEERS):
                read(tile, kv, offset).start()

    @pl.loop(0, tiles)
    def _(tile):
        start = first + tile * block
        plain = (start + block <= row_len) & ((new_slot < start) | (new_slot >= start + block))
        for kv in range(2):
            for offset in range(PEERS):
                read(tile, kv, offset).wait()

            def group(at):
                return jnp.swapaxes(held[tile, kv, :, at:at + GROUP, :], 0, 1).reshape(GROUP * PEERS, -1)

            @pl.when(plain)
            def _():
                for at in range(0, block, GROUP):
                    mixed[tile, kv, at * PEERS:(at + GROUP) * PEERS, :] = group(at)

            @pl.when(jnp.logical_not(plain))
            def _():
                new = jnp.concatenate([new_ref[kv]] * GROUP, axis=0)
                slot_of_row = lax.broadcasted_iota(jnp.int32, new.shape, 0) // PEERS
                for at in range(0, block, GROUP):
                    slots = slot_of_row + (start + at)
                    rows = jnp.where(slots < row_len, group(at).astype(jnp.float32), 0.0)
                    rows = jnp.where(slots == new_slot, new, rows)
                    mixed[tile, kv, at * PEERS:(at + GROUP) * PEERS, :] = rows.astype(jnp.bfloat16)

            write(tile, kv).start()

    @pl.loop(0, tiles)
    def _(tile):
        for kv in range(2):
            write(tile, kv).wait()


def interleave(first, row_len, new, own, pieces, caches):
    count, dim = pieces[0].shape[1:]
    block = BLOCK if count % BLOCK == 0 else BLOCK // 2
    tiles = count // block
    cache = jax.ShapeDtypeStruct((WINDOW * PEERS, dim), jnp.bfloat16)
    any_spec = pl.BlockSpec(memory_space=pltpu.HBM)
    args = [row_len, new, *own, *pieces]
    in_specs = [pl.BlockSpec(memory_space=pltpu.SMEM)] + [pl.BlockSpec(memory_space=pltpu.VMEM)] + [any_spec] * (len(own) + len(pieces))
    aliases = {}
    if caches is not None:
        aliases = {len(args): 0, len(args) + 1: 1}
        args += caches
        in_specs += [any_spec] * 2
    return pl.pallas_call(
        functools.partial(interleave_kernel, first, count, block, len(own) == 2, len(aliases)),
        out_shape=[cache, cache],
        in_specs=in_specs,
        out_specs=[any_spec] * 2,
        input_output_aliases=aliases,
        scratch_shapes=[
            pltpu.VMEM((tiles, 2, PEERS, block, dim), jnp.bfloat16),
            pltpu.VMEM((tiles, 2, block * PEERS, dim), jnp.bfloat16),
            pltpu.SemaphoreType.DMA((tiles, 2, PEERS)),
            pltpu.SemaphoreType.DMA((tiles, 2)),
        ],
        compiler_params=pltpu.CompilerParams(vmem_limit_bytes=VMEM_LIMIT),
        cost_estimate=pl.CostEstimate(flops=count * 64 * dim, bytes_accessed=count * PEERS * dim * 8, transcendentals=0),
    )(*args)


def last_kernel(first, count, new_ref, *refs):
    pieces = refs[:PEERS]
    k_out, v_out, mixed, sems = refs[PEERS + 2:]
    me = lax.axis_index('sh')
    row_len = jnp.concatenate([new_ref[2].astype(jnp.int32)] * GROUP, axis=0)
    new_slot = row_len & (WINDOW - 1)
    by_offset = pieces[-1:] + tuple(pieces[ORDER.index(offset)] for offset in range(1, PEERS))
    copies = []
    for kv, out in enumerate((k_out, v_out)):
        new = jnp.concatenate([new_ref[kv]] * GROUP, axis=0)
        slot_of_row = lax.broadcasted_iota(jnp.int32, new.shape, 0) // PEERS
        for at in range(0, count, GROUP):
            heads = [ref[kv, at:at + GROUP, :] for ref in by_offset]
            for bit in (1, 2, 4):
                swapped = (me & bit) != 0
                heads = [jnp.where(swapped, heads[head ^ bit], heads[head]) for head in range(PEERS)]
            rows = jnp.swapaxes(jnp.stack(heads, axis=0), 0, 1).reshape(GROUP * PEERS, -1)
            slots = slot_of_row + (first + at)
            rows = jnp.where(slots < row_len, rows.astype(jnp.float32), 0.0)
            rows = jnp.where(slots == new_slot, new, rows)
            mixed[kv, at * PEERS:(at + GROUP) * PEERS, :] = rows.astype(jnp.bfloat16)
        copies.append(pltpu.make_async_copy(mixed.at[kv], out.at[pl.ds(first * PEERS, count * PEERS)], sems.at[kv]))
        copies[-1].start()
    for copy in copies:
        copy.wait()


def interleave_last(first, new, pieces, caches):
    count, dim = pieces[0].shape[1:]
    cache = jax.ShapeDtypeStruct((WINDOW * PEERS, dim), jnp.bfloat16)
    return pl.pallas_call(
        functools.partial(last_kernel, first, count),
        out_shape=[cache, cache],
        in_specs=[pl.BlockSpec(memory_space=pltpu.VMEM)] * (1 + PEERS) + [pl.BlockSpec(memory_space=pltpu.HBM)] * 2,
        out_specs=[pl.BlockSpec(memory_space=pltpu.HBM)] * 2,
        input_output_aliases={1 + PEERS: 0, 2 + PEERS: 1},
        scratch_shapes=[pltpu.VMEM((2, count * PEERS, dim), jnp.bfloat16), pltpu.SemaphoreType.DMA((2,))],
        compiler_params=pltpu.CompilerParams(vmem_limit_bytes=LAST_VMEM_LIMIT),
        cost_estimate=pl.CostEstimate(flops=count * 64 * dim, bytes_accessed=count * PEERS * dim * 8, transcendentals=0),
    )(new, *pieces, *caches)


def solution(mesh):
    head_spec = P('dp', None, 'sh', None)
    row_spec = P(('dp', 'sh'))
    full_spec = P(None, None)

    def swap(value, offset):
        return lax.ppermute(value, 'sh', [(i, i ^ offset) for i in range(PEERS)])

    def exchange(table, me):
        got = [lax.dynamic_slice_in_dim(table, me ^ offset, 1) for offset in range(PEERS)]
        return [got[0]] + [swap(got[offset], offset) for offset in range(1, PEERS)]

    def by_device(got, me):
        return jnp.take(jnp.concatenate(got, axis=0), me ^ jnp.arange(PEERS), axis=0)

    def per_device(k_prefill, v_prefill, lengths, residual, norm_gain, w_query, w_key, w_value, w_out):
        me = lax.axis_index('sh')
        seq_len = k_prefill.shape[1]
        head_dim = k_prefill.shape[3]
        k_mine = k_prefill.reshape(PEERS, seq_len, head_dim)
        v_mine = v_prefill.reshape(PEERS, seq_len, head_dim)
        my_len = lax.dynamic_slice_in_dim(lengths, me, 1)
        received = {}

        def send(first, pieces):
            received[first] = [swap(piece, offset) for piece, offset in zip(pieces, ORDER)]

        def start(chunk, after=None, before=None):
            prefills = (k_mine, v_mine)
            if after is not None:
                prefills, after = lax.optimization_barrier((prefills, after))
            pieces = pack(*chunk, chunk == CHUNKS[-1], *prefills)
            pieces, before = lax.optimization_barrier((pieces, before))
            send(chunk[0], pieces)
            received[chunk[0]] += pieces[len(ORDER):]
            return after, before

        _, residual = start(CHUNKS[0], before=residual)
        _, residual = start(CHUNKS[1], after=residual, before=residual)

        resid_f32 = residual.astype(jnp.float32)
        inv_rms = lax.rsqrt(jnp.mean(resid_f32 * resid_f32, axis=-1, keepdims=True) + EPS)
        normed = (resid_f32 * inv_rms * norm_gain.astype(jnp.float32)).astype(jnp.bfloat16)
        q_heads = jnp.dot(normed, w_query, preferred_element_type=jnp.float32).astype(jnp.bfloat16).reshape(1, -1, head_dim)
        k_new = jnp.dot(normed, w_key, preferred_element_type=jnp.float32).astype(jnp.bfloat16).reshape(1, PEERS, head_dim)
        v_new = jnp.dot(normed, w_value, preferred_element_type=jnp.float32).astype(jnp.bfloat16).reshape(1, PEERS, head_dim)
        q_heads = rotate(q_heads, my_len)
        k_new = rotate(k_new, my_len)
        q_group = q_heads.shape[1] // PEERS
        new = jnp.concatenate([k_new.astype(jnp.float32), v_new.astype(jnp.float32), jnp.broadcast_to(my_len.astype(jnp.float32), (1, PEERS, head_dim))], axis=0)

        table = jnp.concatenate([q_heads.reshape(PEERS, q_group, head_dim), k_new.reshape(PEERS, 1, head_dim), v_new.reshape(PEERS, 1, head_dim)], axis=1).reshape(PEERS, -1)
        qkv_parts = exchange(table, me)
        _, table = start(CHUNKS[2], after=table, before=table)
        wrap_lengths, _ = lax.optimization_barrier((lengths, table))
        wrapped = wrap_pack(wrap_lengths, k_mine, v_mine)
        send(0, wrapped[:-1])
        qkv = by_device(qkv_parts, me).reshape(PEERS, q_group + 2, head_dim)
        q_all, k_all, v_all = qkv[:, :q_group], qkv[:, q_group:q_group + 1], qkv[:, q_group + 1:]
        positions = jnp.arange(seq_len, dtype=jnp.int32)[None, :]
        live = (positions < lengths[:, None]) & (positions > lengths[:, None] - WINDOW)
        scores = jnp.einsum('bgd,bsd->bgs', q_all, k_mine, preferred_element_type=jnp.float32) / head_dim ** 0.5
        scores = jnp.where(live[:, None, :], scores, -jnp.inf)
        top_old = jnp.max(scores, axis=-1, keepdims=True)
        new_score = jnp.sum(q_all.astype(jnp.float32) * k_all.astype(jnp.float32), axis=-1, keepdims=True) / head_dim ** 0.5
        top = jnp.maximum(top_old, new_score)
        exp_scores = jnp.exp(scores - top)
        exp_new = jnp.exp(new_score - top)
        total = jnp.sum(exp_scores, axis=-1, keepdims=True) + exp_new
        weights = (exp_scores / total).astype(jnp.bfloat16)
        new_weight = lax.reduce_precision(exp_new / total, 8, 7)
        mixed = jnp.einsum('bgs,bsd->bgd', weights, v_mine, preferred_element_type=jnp.float32)
        mixed = (mixed + new_weight * v_all.astype(jnp.float32)).astype(jnp.bfloat16).reshape(PEERS, -1)
        attn_parts = exchange(mixed, me)

        place_len, _ = lax.optimization_barrier((my_len, mixed))
        caches = None

        def store(first, caches):
            own = [wrapped[-1]] if first == 0 else [k_mine, v_mine]
            if first == CHUNKS[-1][0]:
                return interleave_last(first, new, received[first], caches)
            return interleave(first, place_len, new, own, received[first], caches)

        caches = store(CHUNKS[0][0], caches)
        caches = store(CHUNKS[1][0], caches)
        caches, caches = start(CHUNKS[3], after=caches, before=caches)
        caches, caches = start(CHUNKS[4], after=caches, before=caches)
        caches = store(CHUNKS[2][0], caches)
        caches, caches = start(CHUNKS[5], after=caches, before=caches)
        attn_parts, caches = lax.optimization_barrier((attn_parts, caches))
        attn_out = by_device(attn_parts, me).reshape(1, -1)
        resid_out = (resid_f32 + jnp.dot(attn_out, w_out, preferred_element_type=jnp.float32)).astype(jnp.bfloat16)
        for first in (0,) + tuple(chunk[0] for chunk in CHUNKS[3:]):
            caches = store(first, caches)
        shape = (1, WINDOW, PEERS, head_dim)
        return resid_out, caches[0].reshape(shape), caches[1].reshape(shape)

    return jax.shard_map(per_device, mesh=mesh, in_specs=(head_spec, head_spec, P('dp'), P(('dp', 'sh'), None), P(None), full_spec, full_spec, full_spec, full_spec), out_specs=(P(('dp', 'sh'), None), row_spec, row_spec), check_vma=False)
```

```python
import functools

import jax
import jax.numpy as jnp
from jax import lax
from jax.experimental import pallas as pl
from jax.experimental.pallas import tpu as pltpu
from jax.sharding import PartitionSpec as P


WINDOW = 4096
THETA = 10000.0
EPS = 1e-5
PEERS = 8
GROUP = 32
WRAP = 256
CHUNKS = ((256, 512), (768, 1024), (1792, 1280), (3072, 640), (3712, 256), (3968, 128))
BLOCK = 256
ORDER = (6, 4, 2, 7, 5, 3, 1)
VMEM_LIMIT = 56 * 1024 * 1024
LAST_VMEM_LIMIT = 8 * 1024 * 1024


def rotate(heads, positions):
    head_dim = heads.shape[-1]
    half_dim = head_dim // 2
    inv_freq = THETA ** (-2.0 * jnp.arange(half_dim, dtype=jnp.float32) / head_dim)
    angles = positions.astype(jnp.float32).reshape(positions.shape + (1,) * (heads.ndim - 1)) * inv_freq
    cos_part = jnp.cos(angles)
    sin_part = jnp.sin(angles)
    first_half = heads[..., :half_dim].astype(jnp.float32)
    second_half = heads[..., half_dim:].astype(jnp.float32)
    return jnp.concatenate([first_half * cos_part - second_half * sin_part, second_half * cos_part + first_half * sin_part], axis=-1).astype(jnp.bfloat16)


def pack_kernel(first, count, offsets, k_ref, v_ref, *refs):
    outs, sems = refs[:-1], refs[-1]
    me = lax.axis_index('sh')
    copies = []
    for at, offset in enumerate(offsets):
        for kv, src in enumerate((k_ref, v_ref)):
            copies.append(pltpu.make_async_copy(src.at[me ^ offset, pl.ds(first, count)], outs[at].at[kv], sems.at[at, kv]))
            copies[-1].start()
    for copy in copies:
        copy.wait()


def pack(first, count, offsets, k_mine, v_mine):
    dim = k_mine.shape[2]
    pieces = len(offsets)
    return pl.pallas_call(
        functools.partial(pack_kernel, first, count, offsets),
        out_shape=[jax.ShapeDtypeStruct((2, count, dim), jnp.bfloat16)] * pieces,
        in_specs=[pl.BlockSpec(memory_space=pltpu.HBM)] * 2,
        out_specs=[pl.BlockSpec(memory_space=pltpu.VMEM)] * pieces,
        scratch_shapes=[pltpu.SemaphoreType.DMA((pieces, 2))],
        compiler_params=pltpu.CompilerParams(vmem_limit_bytes=VMEM_LIMIT),
        cost_estimate=pl.CostEstimate(flops=0, bytes_accessed=pieces * 4 * count * dim * 2, transcendentals=0),
    )(k_mine, v_mine)


def wrap_kernel(len_ref, k_ref, k_late_ref, v_ref, v_late_ref, *outs):
    me = lax.axis_index('sh')
    slots = lax.broadcasted_iota(jnp.int32, (WRAP, 128), 0)
    for out, offset in zip(outs, ORDER + (0,)):
        row = me ^ offset
        late = slots + WINDOW < len_ref[row]
        for kv, (base_ref, late_ref) in enumerate(((k_ref, k_late_ref), (v_ref, v_late_ref))):
            out[kv] = jnp.where(late, late_ref[row].astype(jnp.float32), base_ref[row].astype(jnp.float32)).astype(jnp.bfloat16)


def wrap_pack(lengths, k_mine, v_mine):
    rows, _, dim = k_mine.shape
    base = pl.BlockSpec((rows, WRAP, dim), lambda i: (0, 0, 0))
    late = pl.BlockSpec((rows, WRAP, dim), lambda i: (0, WINDOW // WRAP, 0))
    piece = jax.ShapeDtypeStruct((2, WRAP, dim), jnp.bfloat16)
    return pl.pallas_call(
        wrap_kernel,
        grid=(1,),
        out_shape=[piece] * (len(ORDER) + 1),
        out_specs=[pl.BlockSpec((2, WRAP, dim), lambda i: (0, 0, 0))] * (len(ORDER) + 1),
        in_specs=[pl.BlockSpec(memory_space=pltpu.SMEM), base, late, base, late],
        compiler_params=pltpu.CompilerParams(vmem_limit_bytes=VMEM_LIMIT),
        cost_estimate=pl.CostEstimate(flops=rows * 8 * WRAP * dim, bytes_accessed=rows * 6 * WRAP * dim * 2, transcendentals=0),
    )(lengths, k_mine, k_mine, v_mine, v_mine)


def interleave_kernel(first, count, block, has_own, num_alias, len_ref, new_ref, *refs):
    num_own = 2 if has_own else 1
    own = refs[:num_own]
    pieces = refs[num_own:num_own + len(ORDER)]
    k_out, v_out, held, mixed, in_sems, out_sems = refs[num_own + len(ORDER) + num_alias:]
    tiles = count // block
    me = lax.axis_index('sh')
    row_len = len_ref[0]
    new_slot = lax.rem(row_len, WINDOW)
    outs = (k_out, v_out)

    def read(tile, kv, offset):
        at = pl.multiple_of(tile * block, block)
        if offset:
            src = pieces[ORDER.index(offset)].at[kv, pl.ds(at, block)]
        elif has_own:
            src = own[kv].at[me, pl.ds(first + at, block)]
        else:
            src = own[0].at[kv, pl.ds(at, block)]
        return pltpu.make_async_copy(src, held.at[tile, kv, me ^ offset], in_sems.at[tile, kv, offset])

    def write(tile, kv):
        at = pl.multiple_of((first + tile * block) * PEERS, block * PEERS)
        return pltpu.make_async_copy(mixed.at[tile, kv], outs[kv].at[pl.ds(at, block * PEERS)], out_sems.at[tile, kv])

    @pl.loop(0, tiles)
    def _(tile):
        for kv in range(2):
            for offset in range(PEERS):
                read(tile, kv, offset).start()

    @pl.loop(0, tiles)
    def _(tile):
        start = first + tile * block
        plain = (start + block <= row_len) & ((new_slot < start) | (new_slot >= start + block))
        for kv in range(2):
            for offset in range(PEERS):
                read(tile, kv, offset).wait()

            def group(at):
                return jnp.swapaxes(held[tile, kv, :, at:at + GROUP, :], 0, 1).reshape(GROUP * PEERS, -1)

            @pl.when(plain)
            def _():
                for at in range(0, block, GROUP):
                    mixed[tile, kv, at * PEERS:(at + GROUP) * PEERS, :] = group(at)

            @pl.when(jnp.logical_not(plain))
            def _():
                new = jnp.concatenate([new_ref[kv]] * GROUP, axis=0)
                slot_of_row = lax.broadcasted_iota(jnp.int32, new.shape, 0) // PEERS
                for at in range(0, block, GROUP):
                    slots = slot_of_row + (start + at)
                    rows = jnp.where(slots < row_len, group(at).astype(jnp.float32), 0.0)
                    rows = jnp.where(slots == new_slot, new, rows)
                    mixed[tile, kv, at * PEERS:(at + GROUP) * PEERS, :] = rows.astype(jnp.bfloat16)

            write(tile, kv).start()

    @pl.loop(0, tiles)
    def _(tile):
        for kv in range(2):
            write(tile, kv).wait()


def interleave(first, row_len, new, own, pieces, caches):
    count, dim = pieces[0].shape[1:]
    block = BLOCK if count % BLOCK == 0 else BLOCK // 2
    tiles = count // block
    cache = jax.ShapeDtypeStruct((WINDOW * PEERS, dim), jnp.bfloat16)
    any_spec = pl.BlockSpec(memory_space=pltpu.HBM)
    args = [row_len, new, *own, *pieces]
    in_specs = [pl.BlockSpec(memory_space=pltpu.SMEM)] + [pl.BlockSpec(memory_space=pltpu.VMEM)] + [any_spec] * (len(own) + len(pieces))
    aliases = {}
    if caches is not None:
        aliases = {len(args): 0, len(args) + 1: 1}
        args += caches
        in_specs += [any_spec] * 2
    return pl.pallas_call(
        functools.partial(interleave_kernel, first, count, block, len(own) == 2, len(aliases)),
        out_shape=[cache, cache],
        in_specs=in_specs,
        out_specs=[any_spec] * 2,
        input_output_aliases=aliases,
        scratch_shapes=[
            pltpu.VMEM((tiles, 2, PEERS, block, dim), jnp.bfloat16),
            pltpu.VMEM((tiles, 2, block * PEERS, dim), jnp.bfloat16),
            pltpu.SemaphoreType.DMA((tiles, 2, PEERS)),
            pltpu.SemaphoreType.DMA((tiles, 2)),
        ],
        compiler_params=pltpu.CompilerParams(vmem_limit_bytes=VMEM_LIMIT),
        cost_estimate=pl.CostEstimate(flops=count * 64 * dim, bytes_accessed=count * PEERS * dim * 8, transcendentals=0),
    )(*args)


def last_kernel(first, count, new_ref, *refs):
    pieces = refs[:PEERS]
    k_out, v_out, mixed, sems = refs[PEERS + 2:]
    me = lax.axis_index('sh')
    row_len = jnp.concatenate([new_ref[2].astype(jnp.int32)] * GROUP, axis=0)
    new_slot = row_len & (WINDOW - 1)
    by_offset = pieces[-1:] + tuple(pieces[ORDER.index(offset)] for offset in range(1, PEERS))
    copies = []
    for kv, out in enumerate((k_out, v_out)):
        new = jnp.concatenate([new_ref[kv]] * GROUP, axis=0)
        slot_of_row = lax.broadcasted_iota(jnp.int32, new.shape, 0) // PEERS
        for at in range(0, count, GROUP):
            heads = [ref[kv, at:at + GROUP, :] for ref in by_offset]
            for bit in (1, 2, 4):
                swapped = (me & bit) != 0
                heads = [jnp.where(swapped, heads[head ^ bit], heads[head]) for head in range(PEERS)]
            rows = jnp.swapaxes(jnp.stack(heads, axis=0), 0, 1).reshape(GROUP * PEERS, -1)
            slots = slot_of_row + (first + at)
            rows = jnp.where(slots < row_len, rows.astype(jnp.float32), 0.0)
            rows = jnp.where(slots == new_slot, new, rows)
            mixed[kv, at * PEERS:(at + GROUP) * PEERS, :] = rows.astype(jnp.bfloat16)
        copies.append(pltpu.make_async_copy(mixed.at[kv], out.at[pl.ds(first * PEERS, count * PEERS)], sems.at[kv]))
        copies[-1].start()
    for copy in copies:
        copy.wait()


def interleave_last(first, new, pieces, caches):
    count, dim = pieces[0].shape[1:]
    cache = jax.ShapeDtypeStruct((WINDOW * PEERS, dim), jnp.bfloat16)
    return pl.pallas_call(
        functools.partial(last_kernel, first, count),
        out_shape=[cache, cache],
        in_specs=[pl.BlockSpec(memory_space=pltpu.VMEM)] * (1 + PEERS) + [pl.BlockSpec(memory_space=pltpu.HBM)] * 2,
        out_specs=[pl.BlockSpec(memory_space=pltpu.HBM)] * 2,
        input_output_aliases={1 + PEERS: 0, 2 + PEERS: 1},
        scratch_shapes=[pltpu.VMEM((2, count * PEERS, dim), jnp.bfloat16), pltpu.SemaphoreType.DMA((2,))],
        compiler_params=pltpu.CompilerParams(vmem_limit_bytes=LAST_VMEM_LIMIT),
        cost_estimate=pl.CostEstimate(flops=count * 64 * dim, bytes_accessed=count * PEERS * dim * 8, transcendentals=0),
    )(new, *pieces, *caches)


def solution(mesh):
    head_spec = P('dp', None, 'sh', None)
    row_spec = P(('dp', 'sh'))
    full_spec = P(None, None)

    def swap(value, offset):
        return lax.ppermute(value, 'sh', [(i, i ^ offset) for i in range(PEERS)])

    def exchange(table, me):
        got = [lax.dynamic_slice_in_dim(table, me ^ offset, 1) for offset in range(PEERS)]
        return [got[0]] + [swap(got[offset], offset) for offset in range(1, PEERS)]

    def by_device(got, me):
        return jnp.take(jnp.concatenate(got, axis=0), me ^ jnp.arange(PEERS), axis=0)

    def per_device(k_prefill, v_prefill, lengths, residual, norm_gain, w_query, w_key, w_value, w_out):
        me = lax.axis_index('sh')
        seq_len = k_prefill.shape[1]
        head_dim = k_prefill.shape[3]
        k_mine = k_prefill.reshape(PEERS, seq_len, head_dim)
        v_mine = v_prefill.reshape(PEERS, seq_len, head_dim)
        my_len = lax.dynamic_slice_in_dim(lengths, me, 1)
        received = {}

        def send(first, pieces, offsets=ORDER):
            received[first] = received.get(first, []) + [swap(piece, offset) for piece, offset in zip(pieces, offsets)]

        def start(chunk, after=None, before=None, offsets=ORDER):
            prefills = (k_mine, v_mine)
            if after is not None:
                prefills, after = lax.optimization_barrier((prefills, after))
            own = (0,) * (chunk == CHUNKS[-1])
            pieces = pack(*chunk, offsets + own, *prefills)
            pieces, before = lax.optimization_barrier((pieces, before))
            send(chunk[0], pieces, offsets)
            received[chunk[0]] += pieces[len(offsets):]
            return after, before

        _, residual = start(CHUNKS[0], before=residual, offsets=ORDER[:1])
        _, residual = start(CHUNKS[0], after=residual, before=residual, offsets=ORDER[1:])
        _, residual = start(CHUNKS[1], after=residual, before=residual)

        resid_f32 = residual.astype(jnp.float32)
        inv_rms = lax.rsqrt(jnp.mean(resid_f32 * resid_f32, axis=-1, keepdims=True) + EPS)
        normed = (resid_f32 * inv_rms * norm_gain.astype(jnp.float32)).astype(jnp.bfloat16)
        q_heads = jnp.dot(normed, w_query, preferred_element_type=jnp.float32).astype(jnp.bfloat16).reshape(1, -1, head_dim)
        k_new = jnp.dot(normed, w_key, preferred_element_type=jnp.float32).astype(jnp.bfloat16).reshape(1, PEERS, head_dim)
        v_new = jnp.dot(normed, w_value, preferred_element_type=jnp.float32).astype(jnp.bfloat16).reshape(1, PEERS, head_dim)
        q_heads = rotate(q_heads, my_len)
        k_new = rotate(k_new, my_len)
        q_group = q_heads.shape[1] // PEERS
        new = jnp.concatenate([k_new.astype(jnp.float32), v_new.astype(jnp.float32), jnp.broadcast_to(my_len.astype(jnp.float32), (1, PEERS, head_dim))], axis=0)

        table = jnp.concatenate([q_heads.reshape(PEERS, q_group, head_dim), k_new.reshape(PEERS, 1, head_dim), v_new.reshape(PEERS, 1, head_dim)], axis=1).reshape(PEERS, -1)
        qkv_parts = exchange(table, me)
        _, table = start(CHUNKS[2], after=table, before=table)
        wrap_lengths, _ = lax.optimization_barrier((lengths, table))
        wrapped = wrap_pack(wrap_lengths, k_mine, v_mine)
        send(0, wrapped[:-1])
        qkv = by_device(qkv_parts, me).reshape(PEERS, q_group + 2, head_dim)
        q_all, k_all, v_all = qkv[:, :q_group], qkv[:, q_group:q_group + 1], qkv[:, q_group + 1:]
        positions = jnp.arange(seq_len, dtype=jnp.int32)[None, :]
        live = (positions < lengths[:, None]) & (positions > lengths[:, None] - WINDOW)
        scores = jnp.einsum('bgd,bsd->bgs', q_all, k_mine, preferred_element_type=jnp.float32) / head_dim ** 0.5
        scores = jnp.where(live[:, None, :], scores, -jnp.inf)
        top_old = jnp.max(scores, axis=-1, keepdims=True)
        new_score = jnp.sum(q_all.astype(jnp.float32) * k_all.astype(jnp.float32), axis=-1, keepdims=True) / head_dim ** 0.5
        top = jnp.maximum(top_old, new_score)
        exp_scores = jnp.exp(scores - top)
        exp_new = jnp.exp(new_score - top)
        total = jnp.sum(exp_scores, axis=-1, keepdims=True) + exp_new
        weights = (exp_scores / total).astype(jnp.bfloat16)
        new_weight = lax.reduce_precision(exp_new / total, 8, 7)
        mixed = jnp.einsum('bgs,bsd->bgd', weights, v_mine, preferred_element_type=jnp.float32)
        mixed = (mixed + new_weight * v_all.astype(jnp.float32)).astype(jnp.bfloat16).reshape(PEERS, -1)
        attn_parts = exchange(mixed, me)

        place_len, _ = lax.optimization_barrier((my_len, mixed))
        caches = None

        def store(first, caches):
            own = [wrapped[-1]] if first == 0 else [k_mine, v_mine]
            if first == CHUNKS[-1][0]:
                return interleave_last(first, new, received[first], caches)
            return interleave(first, place_len, new, own, received[first], caches)

        caches = store(CHUNKS[0][0], caches)
        caches = store(CHUNKS[1][0], caches)
        caches, caches = start(CHUNKS[3], after=caches, before=caches)
        caches, caches = start(CHUNKS[4], after=caches, before=caches)
        caches = store(CHUNKS[2][0], caches)
        caches, caches = start(CHUNKS[5], after=caches, before=caches)
        attn_parts, caches = lax.optimization_barrier((attn_parts, caches))
        attn_out = by_device(attn_parts, me).reshape(1, -1)
        resid_out = (resid_f32 + jnp.dot(attn_out, w_out, preferred_element_type=jnp.float32)).astype(jnp.bfloat16)
        for first in (0,) + tuple(chunk[0] for chunk in CHUNKS[3:]):
            caches = store(first, caches)
        shape = (1, WINDOW, PEERS, head_dim)
        return resid_out, caches[0].reshape(shape), caches[1].reshape(shape)

    return jax.shard_map(per_device, mesh=mesh, in_specs=(head_spec, head_spec, P('dp'), P(('dp', 'sh'), None), P(None), full_spec, full_spec, full_spec, full_spec), out_specs=(P(('dp', 'sh'), None), row_spec, row_spec), check_vma=False)
```

```python
import functools

import jax
import jax.numpy as jnp
from jax import lax
from jax.experimental import pallas as pl
from jax.experimental.pallas import tpu as pltpu
from jax.sharding import PartitionSpec as P


WINDOW = 4096
THETA = 10000.0
EPS = 1e-5
PEERS = 8
GROUP = 32
WRAP = 256
SMALL = 256
CHUNKS = ((256, 512), (768, 1024), (1792, 1280), (3072, 640), (3712, 256), (3968, 128))
BLOCK = 256
ORDER = (6, 4, 2, 7, 5, 3, 1)
VMEM_LIMIT = 56 * 1024 * 1024
SMALL_VMEM_LIMIT = 8 * 1024 * 1024


def rotate(heads, positions):
    head_dim = heads.shape[-1]
    half_dim = head_dim // 2
    inv_freq = THETA ** (-2.0 * jnp.arange(half_dim, dtype=jnp.float32) / head_dim)
    angles = positions.astype(jnp.float32).reshape(positions.shape + (1,) * (heads.ndim - 1)) * inv_freq
    cos_part = jnp.cos(angles)
    sin_part = jnp.sin(angles)
    first_half = heads[..., :half_dim].astype(jnp.float32)
    second_half = heads[..., half_dim:].astype(jnp.float32)
    return jnp.concatenate([first_half * cos_part - second_half * sin_part, second_half * cos_part + first_half * sin_part], axis=-1).astype(jnp.bfloat16)


def pack_kernel(first, count, offsets, k_ref, v_ref, *refs):
    outs, sems = refs[:-1], refs[-1]
    me = lax.axis_index('sh')
    copies = []
    for at, offset in enumerate(offsets):
        for kv, src in enumerate((k_ref, v_ref)):
            copies.append(pltpu.make_async_copy(src.at[me ^ offset, pl.ds(first, count)], outs[at].at[kv], sems.at[at, kv]))
            copies[-1].start()
    for copy in copies:
        copy.wait()


def pack(first, count, offsets, k_mine, v_mine):
    dim = k_mine.shape[2]
    pieces = len(offsets)
    return pl.pallas_call(
        functools.partial(pack_kernel, first, count, offsets),
        out_shape=[jax.ShapeDtypeStruct((2, count, dim), jnp.bfloat16)] * pieces,
        in_specs=[pl.BlockSpec(memory_space=pltpu.HBM)] * 2,
        out_specs=[pl.BlockSpec(memory_space=pltpu.VMEM)] * pieces,
        scratch_shapes=[pltpu.SemaphoreType.DMA((pieces, 2))],
        compiler_params=pltpu.CompilerParams(vmem_limit_bytes=VMEM_LIMIT),
        cost_estimate=pl.CostEstimate(flops=0, bytes_accessed=pieces * 4 * count * dim * 2, transcendentals=0),
    )(k_mine, v_mine)


def wrap_kernel(len_ref, k_ref, k_late_ref, v_ref, v_late_ref, *outs):
    me = lax.axis_index('sh')
    slots = lax.broadcasted_iota(jnp.int32, (WRAP, 128), 0)
    for out, offset in zip(outs, ORDER + (0,)):
        row = me ^ offset
        late = slots + WINDOW < len_ref[row]
        for kv, (base_ref, late_ref) in enumerate(((k_ref, k_late_ref), (v_ref, v_late_ref))):
            out[kv] = jnp.where(late, late_ref[row].astype(jnp.float32), base_ref[row].astype(jnp.float32)).astype(jnp.bfloat16)


def wrap_pack(lengths, k_mine, v_mine):
    rows, _, dim = k_mine.shape
    base = pl.BlockSpec((rows, WRAP, dim), lambda i: (0, 0, 0))
    late = pl.BlockSpec((rows, WRAP, dim), lambda i: (0, WINDOW // WRAP, 0))
    piece = jax.ShapeDtypeStruct((2, WRAP, dim), jnp.bfloat16)
    return pl.pallas_call(
        wrap_kernel,
        grid=(1,),
        out_shape=[piece] * (len(ORDER) + 1),
        out_specs=[pl.BlockSpec((2, WRAP, dim), lambda i: (0, 0, 0))] * (len(ORDER) + 1),
        in_specs=[pl.BlockSpec(memory_space=pltpu.SMEM), base, late, base, late],
        compiler_params=pltpu.CompilerParams(vmem_limit_bytes=VMEM_LIMIT),
        cost_estimate=pl.CostEstimate(flops=rows * 8 * WRAP * dim, bytes_accessed=rows * 6 * WRAP * dim * 2, transcendentals=0),
    )(lengths, k_mine, k_mine, v_mine, v_mine)


def interleave_kernel(first, count, block, lead, num_alias, len_ref, new_ref, *refs):
    own = refs[:2]
    num_pieces = len(ORDER) + lead
    pieces = refs[2:2 + num_pieces]
    k_out, v_out, held, mixed, in_sems, out_sems = refs[2 + num_pieces + num_alias:]
    tiles = count // block
    me = lax.axis_index('sh')
    row_len = len_ref[0]
    new_slot = lax.rem(row_len, WINDOW)
    outs = (k_out, v_out)

    def read(tile, kv, offset):
        at = pl.multiple_of(tile * block, block)
        if lead and offset == ORDER[0]:
            src = pieces[kv].at[0, pl.ds(at, block)]
        elif offset:
            src = pieces[ORDER.index(offset) + lead].at[kv, pl.ds(at, block)]
        else:
            src = own[kv].at[me, pl.ds(first + at, block)]
        return pltpu.make_async_copy(src, held.at[tile, kv, me ^ offset], in_sems.at[tile, kv, offset])

    def write(tile, kv):
        at = pl.multiple_of((first + tile * block) * PEERS, block * PEERS)
        return pltpu.make_async_copy(mixed.at[tile, kv], outs[kv].at[pl.ds(at, block * PEERS)], out_sems.at[tile, kv])

    @pl.loop(0, tiles)
    def _(tile):
        for kv in range(2):
            for offset in range(PEERS):
                read(tile, kv, offset).start()

    @pl.loop(0, tiles)
    def _(tile):
        start = first + tile * block
        plain = (start + block <= row_len) & ((new_slot < start) | (new_slot >= start + block))
        for kv in range(2):
            for offset in range(PEERS):
                read(tile, kv, offset).wait()

            def group(at):
                return jnp.swapaxes(held[tile, kv, :, at:at + GROUP, :], 0, 1).reshape(GROUP * PEERS, -1)

            @pl.when(plain)
            def _():
                for at in range(0, block, GROUP):
                    mixed[tile, kv, at * PEERS:(at + GROUP) * PEERS, :] = group(at)

            @pl.when(jnp.logical_not(plain))
            def _():
                new = jnp.concatenate([new_ref[kv]] * GROUP, axis=0)
                slot_of_row = lax.broadcasted_iota(jnp.int32, new.shape, 0) // PEERS
                for at in range(0, block, GROUP):
                    slots = slot_of_row + (start + at)
                    rows = jnp.where(slots < row_len, group(at).astype(jnp.float32), 0.0)
                    rows = jnp.where(slots == new_slot, new, rows)
                    mixed[tile, kv, at * PEERS:(at + GROUP) * PEERS, :] = rows.astype(jnp.bfloat16)

            write(tile, kv).start()

    @pl.loop(0, tiles)
    def _(tile):
        for kv in range(2):
            write(tile, kv).wait()


def interleave(first, row_len, new, own, pieces, caches):
    count, dim = pieces[0].shape[1:]
    lead = len(pieces) - len(ORDER)
    block = BLOCK if count % BLOCK == 0 else BLOCK // 2
    tiles = count // block
    cache = jax.ShapeDtypeStruct((WINDOW * PEERS, dim), jnp.bfloat16)
    any_spec = pl.BlockSpec(memory_space=pltpu.HBM)
    args = [row_len, new, *own, *pieces]
    in_specs = [pl.BlockSpec(memory_space=pltpu.SMEM)] + [pl.BlockSpec(memory_space=pltpu.VMEM)] + [any_spec] * (len(own) + len(pieces))
    aliases = {}
    if caches is not None:
        aliases = {len(args): 0, len(args) + 1: 1}
        args += caches
        in_specs += [any_spec] * 2
    return pl.pallas_call(
        functools.partial(interleave_kernel, first, count, block, lead, len(aliases)),
        out_shape=[cache, cache],
        in_specs=in_specs,
        out_specs=[any_spec] * 2,
        input_output_aliases=aliases,
        scratch_shapes=[
            pltpu.VMEM((tiles, 2, PEERS, block, dim), jnp.bfloat16),
            pltpu.VMEM((tiles, 2, block * PEERS, dim), jnp.bfloat16),
            pltpu.SemaphoreType.DMA((tiles, 2, PEERS)),
            pltpu.SemaphoreType.DMA((tiles, 2)),
        ],
        compiler_params=pltpu.CompilerParams(vmem_limit_bytes=VMEM_LIMIT),
        cost_estimate=pl.CostEstimate(flops=count * 64 * dim, bytes_accessed=count * PEERS * dim * 8, transcendentals=0),
    )(*args)


def small_kernel(first, count, new_ref, *refs):
    pieces = refs[:PEERS]
    k_out, v_out, mixed, sems = refs[PEERS + 2:]
    me = lax.axis_index('sh')
    row_len = jnp.concatenate([new_ref[2].astype(jnp.int32)] * GROUP, axis=0)
    new_slot = row_len & (WINDOW - 1)
    by_offset = pieces[-1:] + tuple(pieces[ORDER.index(offset)] for offset in range(1, PEERS))
    copies = []
    for kv, out in enumerate((k_out, v_out)):
        new = jnp.concatenate([new_ref[kv]] * GROUP, axis=0)
        slot_of_row = lax.broadcasted_iota(jnp.int32, new.shape, 0) // PEERS
        for at in range(0, count, GROUP):
            heads = [ref[kv, at:at + GROUP, :] for ref in by_offset]
            for bit in (1, 2, 4):
                swapped = (me & bit) != 0
                heads = [jnp.where(swapped, heads[head ^ bit], heads[head]) for head in range(PEERS)]
            rows = jnp.swapaxes(jnp.stack(heads, axis=0), 0, 1).reshape(GROUP * PEERS, -1)
            slots = slot_of_row + (first + at)
            rows = jnp.where(slots < row_len, rows.astype(jnp.float32), 0.0)
            rows = jnp.where(slots == new_slot, new, rows)
            mixed[kv, at * PEERS:(at + GROUP) * PEERS, :] = rows.astype(jnp.bfloat16)
        copies.append(pltpu.make_async_copy(mixed.at[kv], out.at[pl.ds(first * PEERS, count * PEERS)], sems.at[kv]))
        copies[-1].start()
    for copy in copies:
        copy.wait()


def interleave_small(first, new, pieces, caches):
    count, dim = pieces[0].shape[1:]
    cache = jax.ShapeDtypeStruct((WINDOW * PEERS, dim), jnp.bfloat16)
    return pl.pallas_call(
        functools.partial(small_kernel, first, count),
        out_shape=[cache, cache],
        in_specs=[pl.BlockSpec(memory_space=pltpu.VMEM)] * (1 + PEERS) + [pl.BlockSpec(memory_space=pltpu.HBM)] * 2,
        out_specs=[pl.BlockSpec(memory_space=pltpu.HBM)] * 2,
        input_output_aliases={1 + PEERS: 0, 2 + PEERS: 1},
        scratch_shapes=[pltpu.VMEM((2, count * PEERS, dim), jnp.bfloat16), pltpu.SemaphoreType.DMA((2,))],
        compiler_params=pltpu.CompilerParams(vmem_limit_bytes=SMALL_VMEM_LIMIT),
        cost_estimate=pl.CostEstimate(flops=count * 64 * dim, bytes_accessed=count * PEERS * dim * 8, transcendentals=0),
    )(new, *pieces, *caches)


def solution(mesh):
    head_spec = P('dp', None, 'sh', None)
    row_spec = P(('dp', 'sh'))
    full_spec = P(None, None)

    def swap(value, offset):
        return lax.ppermute(value, 'sh', [(i, i ^ offset) for i in range(PEERS)])

    def exchange(table, me):
        got = [lax.dynamic_slice_in_dim(table, me ^ offset, 1) for offset in range(PEERS)]
        return [got[0]] + [swap(got[offset], offset) for offset in range(1, PEERS)]

    def by_device(got, me):
        return jnp.take(jnp.concatenate(got, axis=0), me ^ jnp.arange(PEERS), axis=0)

    def per_device(k_prefill, v_prefill, lengths, residual, norm_gain, w_query, w_key, w_value, w_out):
        me = lax.axis_index('sh')
        seq_len = k_prefill.shape[1]
        head_dim = k_prefill.shape[3]
        k_mine = k_prefill.reshape(PEERS, seq_len, head_dim)
        v_mine = v_prefill.reshape(PEERS, seq_len, head_dim)
        my_len = lax.dynamic_slice_in_dim(lengths, me, 1)
        received = {}

        def send(first, pieces, offsets=ORDER):
            received[first] = received.get(first, []) + [swap(piece, offset) for piece, offset in zip(pieces, offsets)]

        def start(chunk, after=None, before=None, offsets=ORDER):
            prefills = (k_mine, v_mine)
            if after is not None:
                prefills, after = lax.optimization_barrier((prefills, after))
            own = (0,) * (chunk[1] <= SMALL and chunk != CHUNKS[0])
            pieces = pack(*chunk, offsets + own, *prefills)
            pieces, before = lax.optimization_barrier((pieces, before))
            send(chunk[0], pieces, offsets)
            received[chunk[0]] += pieces[len(offsets):]
            return after, before

        first, count = CHUNKS[0]
        lead = [lax.dynamic_slice(prefill, (me ^ ORDER[0], first, 0), (1, count, head_dim)) for prefill in (k_mine, v_mine)]
        lead, residual = lax.optimization_barrier((lead, residual))
        send(first, lead, ORDER[:1] * 2)
        _, residual = start(CHUNKS[0], after=residual, before=residual, offsets=ORDER[1:])
        _, residual = start(CHUNKS[1], after=residual, before=residual)

        resid_f32 = residual.astype(jnp.float32)
        inv_rms = lax.rsqrt(jnp.mean(resid_f32 * resid_f32, axis=-1, keepdims=True) + EPS)
        normed = (resid_f32 * inv_rms * norm_gain.astype(jnp.float32)).astype(jnp.bfloat16)
        q_heads = jnp.dot(normed, w_query, preferred_element_type=jnp.float32).astype(jnp.bfloat16).reshape(1, -1, head_dim)
        k_new = jnp.dot(normed, w_key, preferred_element_type=jnp.float32).astype(jnp.bfloat16).reshape(1, PEERS, head_dim)
        v_new = jnp.dot(normed, w_value, preferred_element_type=jnp.float32).astype(jnp.bfloat16).reshape(1, PEERS, head_dim)
        q_heads = rotate(q_heads, my_len)
        k_new = rotate(k_new, my_len)
        q_group = q_heads.shape[1] // PEERS
        new = jnp.concatenate([k_new.astype(jnp.float32), v_new.astype(jnp.float32), jnp.broadcast_to(my_len.astype(jnp.float32), (1, PEERS, head_dim))], axis=0)

        table = jnp.concatenate([q_heads.reshape(PEERS, q_group, head_dim), k_new.reshape(PEERS, 1, head_dim), v_new.reshape(PEERS, 1, head_dim)], axis=1).reshape(PEERS, -1)
        qkv_parts = exchange(table, me)
        _, table = start(CHUNKS[2], after=table, before=table)
        wrap_lengths, _ = lax.optimization_barrier((lengths, table))
        wrapped = wrap_pack(wrap_lengths, k_mine, v_mine)
        send(0, wrapped[:-1])
        received[0] += wrapped[-1:]
        qkv = by_device(qkv_parts, me).reshape(PEERS, q_group + 2, head_dim)
        q_all, k_all, v_all = qkv[:, :q_group], qkv[:, q_group:q_group + 1], qkv[:, q_group + 1:]
        positions = jnp.arange(seq_len, dtype=jnp.int32)[None, :]
        live = (positions < lengths[:, None]) & (positions > lengths[:, None] - WINDOW)
        scores = jnp.einsum('bgd,bsd->bgs', q_all, k_mine, preferred_element_type=jnp.float32) / head_dim ** 0.5
        scores = jnp.where(live[:, None, :], scores, -jnp.inf)
        top_old = jnp.max(scores, axis=-1, keepdims=True)
        new_score = jnp.sum(q_all.astype(jnp.float32) * k_all.astype(jnp.float32), axis=-1, keepdims=True) / head_dim ** 0.5
        top = jnp.maximum(top_old, new_score)
        exp_scores = jnp.exp(scores - top)
        exp_new = jnp.exp(new_score - top)
        total = jnp.sum(exp_scores, axis=-1, keepdims=True) + exp_new
        weights = (exp_scores / total).astype(jnp.bfloat16)
        new_weight = lax.reduce_precision(exp_new / total, 8, 7)
        mixed = jnp.einsum('bgs,bsd->bgd', weights, v_mine, preferred_element_type=jnp.float32)
        mixed = (mixed + new_weight * v_all.astype(jnp.float32)).astype(jnp.bfloat16).reshape(PEERS, -1)
        attn_parts = exchange(mixed, me)

        place_len, _ = lax.optimization_barrier((my_len, mixed))
        caches = None

        def store(first, caches):
            if received[first][0].shape[1] <= SMALL:
                return interleave_small(first, new, received[first], caches)
            return interleave(first, place_len, new, [k_mine, v_mine], received[first], caches)

        caches = store(CHUNKS[0][0], caches)
        caches = store(CHUNKS[1][0], caches)
        caches, caches = start(CHUNKS[3], after=caches, before=caches)
        caches, caches = start(CHUNKS[4], after=caches, before=caches)
        caches = store(CHUNKS[2][0], caches)
        caches, caches = start(CHUNKS[5], after=caches, before=caches)
        attn_parts, caches = lax.optimization_barrier((attn_parts, caches))
        attn_out = by_device(attn_parts, me).reshape(1, -1)
        resid_out = (resid_f32 + jnp.dot(attn_out, w_out, preferred_element_type=jnp.float32)).astype(jnp.bfloat16)
        for first in (0,) + tuple(chunk[0] for chunk in CHUNKS[3:]):
            caches = store(first, caches)
        shape = (1, WINDOW, PEERS, head_dim)
        return resid_out, caches[0].reshape(shape), caches[1].reshape(shape)

    return jax.shard_map(per_device, mesh=mesh, in_specs=(head_spec, head_spec, P('dp'), P(('dp', 'sh'), None), P(None), full_spec, full_spec, full_spec, full_spec), out_specs=(P(('dp', 'sh'), None), row_spec, row_spec), check_vma=False)
```

```python
import functools

import jax
import jax.numpy as jnp
from jax import lax
from jax.experimental import pallas as pl
from jax.experimental.pallas import tpu as pltpu
from jax.sharding import PartitionSpec as P


WINDOW = 4096
THETA = 10000.0
EPS = 1e-5
PEERS = 8
GROUP = 32
WRAP = 256
SMALL = 256
CHUNKS = ((256, 512), (768, 1024), (1792, 1280), (3072, 768), (3840, 192), (4032, 64))
BLOCK = 256
ORDER = (6, 4, 2, 7, 5, 3, 1)
VMEM_LIMIT = 56 * 1024 * 1024
SMALL_VMEM_LIMIT = 8 * 1024 * 1024


def rotate(heads, positions):
    head_dim = heads.shape[-1]
    half_dim = head_dim // 2
    inv_freq = THETA ** (-2.0 * jnp.arange(half_dim, dtype=jnp.float32) / head_dim)
    angles = positions.astype(jnp.float32).reshape(positions.shape + (1,) * (heads.ndim - 1)) * inv_freq
    cos_part = jnp.cos(angles)
    sin_part = jnp.sin(angles)
    first_half = heads[..., :half_dim].astype(jnp.float32)
    second_half = heads[..., half_dim:].astype(jnp.float32)
    return jnp.concatenate([first_half * cos_part - second_half * sin_part, second_half * cos_part + first_half * sin_part], axis=-1).astype(jnp.bfloat16)


def pack_kernel(first, count, offsets, k_ref, v_ref, *refs):
    outs, sems = refs[:-1], refs[-1]
    me = lax.axis_index('sh')
    copies = []
    for at, offset in enumerate(offsets):
        for kv, src in enumerate((k_ref, v_ref)):
            copies.append(pltpu.make_async_copy(src.at[me ^ offset, pl.ds(first, count)], outs[at].at[kv], sems.at[at, kv]))
            copies[-1].start()
    for copy in copies:
        copy.wait()


def pack(first, count, offsets, k_mine, v_mine):
    dim = k_mine.shape[2]
    pieces = len(offsets)
    return pl.pallas_call(
        functools.partial(pack_kernel, first, count, offsets),
        out_shape=[jax.ShapeDtypeStruct((2, count, dim), jnp.bfloat16)] * pieces,
        in_specs=[pl.BlockSpec(memory_space=pltpu.HBM)] * 2,
        out_specs=[pl.BlockSpec(memory_space=pltpu.VMEM)] * pieces,
        scratch_shapes=[pltpu.SemaphoreType.DMA((pieces, 2))],
        compiler_params=pltpu.CompilerParams(vmem_limit_bytes=VMEM_LIMIT),
        cost_estimate=pl.CostEstimate(flops=0, bytes_accessed=pieces * 4 * count * dim * 2, transcendentals=0),
    )(k_mine, v_mine)


def wrap_kernel(len_ref, k_ref, k_late_ref, v_ref, v_late_ref, *outs):
    me = lax.axis_index('sh')
    slots = lax.broadcasted_iota(jnp.int32, (WRAP, 128), 0)
    for out, offset in zip(outs, ORDER + (0,)):
        row = me ^ offset
        late = slots + WINDOW < len_ref[row]
        for kv, (base_ref, late_ref) in enumerate(((k_ref, k_late_ref), (v_ref, v_late_ref))):
            out[kv] = jnp.where(late, late_ref[row].astype(jnp.float32), base_ref[row].astype(jnp.float32)).astype(jnp.bfloat16)


def wrap_pack(lengths, k_mine, v_mine):
    rows, _, dim = k_mine.shape
    base = pl.BlockSpec((rows, WRAP, dim), lambda i: (0, 0, 0))
    late = pl.BlockSpec((rows, WRAP, dim), lambda i: (0, WINDOW // WRAP, 0))
    piece = jax.ShapeDtypeStruct((2, WRAP, dim), jnp.bfloat16)
    return pl.pallas_call(
        wrap_kernel,
        grid=(1,),
        out_shape=[piece] * (len(ORDER) + 1),
        out_specs=[pl.BlockSpec((2, WRAP, dim), lambda i: (0, 0, 0))] * (len(ORDER) + 1),
        in_specs=[pl.BlockSpec(memory_space=pltpu.SMEM), base, late, base, late],
        compiler_params=pltpu.CompilerParams(vmem_limit_bytes=VMEM_LIMIT),
        cost_estimate=pl.CostEstimate(flops=rows * 8 * WRAP * dim, bytes_accessed=rows * 6 * WRAP * dim * 2, transcendentals=0),
    )(lengths, k_mine, k_mine, v_mine, v_mine)


def interleave_kernel(first, count, block, num_alias, len_ref, new_ref, *refs):
    own = refs[:2]
    pieces = refs[2:2 + len(ORDER)]
    k_out, v_out, held, mixed, in_sems, out_sems = refs[2 + len(ORDER) + num_alias:]
    tiles = count // block
    me = lax.axis_index('sh')
    row_len = len_ref[0]
    new_slot = lax.rem(row_len, WINDOW)
    outs = (k_out, v_out)

    def read(tile, kv, offset):
        at = pl.multiple_of(tile * block, block)
        if offset:
            src = pieces[ORDER.index(offset)].at[kv, pl.ds(at, block)]
        else:
            src = own[kv].at[me, pl.ds(first + at, block)]
        return pltpu.make_async_copy(src, held.at[tile, kv, me ^ offset], in_sems.at[tile, kv, offset])

    def write(tile, kv):
        at = pl.multiple_of((first + tile * block) * PEERS, block * PEERS)
        return pltpu.make_async_copy(mixed.at[tile, kv], outs[kv].at[pl.ds(at, block * PEERS)], out_sems.at[tile, kv])

    @pl.loop(0, tiles)
    def _(tile):
        for kv in range(2):
            for offset in range(PEERS):
                read(tile, kv, offset).start()

    @pl.loop(0, tiles)
    def _(tile):
        start = first + tile * block
        plain = (start + block <= row_len) & ((new_slot < start) | (new_slot >= start + block))
        for kv in range(2):
            for offset in range(PEERS):
                read(tile, kv, offset).wait()

            def group(at):
                return jnp.swapaxes(held[tile, kv, :, at:at + GROUP, :], 0, 1).reshape(GROUP * PEERS, -1)

            @pl.when(plain)
            def _():
                for at in range(0, block, GROUP):
                    mixed[tile, kv, at * PEERS:(at + GROUP) * PEERS, :] = group(at)

            @pl.when(jnp.logical_not(plain))
            def _():
                new = jnp.concatenate([new_ref[kv]] * GROUP, axis=0)
                slot_of_row = lax.broadcasted_iota(jnp.int32, new.shape, 0) // PEERS
                for at in range(0, block, GROUP):
                    slots = slot_of_row + (start + at)
                    rows = jnp.where(slots < row_len, group(at).astype(jnp.float32), 0.0)
                    rows = jnp.where(slots == new_slot, new, rows)
                    mixed[tile, kv, at * PEERS:(at + GROUP) * PEERS, :] = rows.astype(jnp.bfloat16)

            write(tile, kv).start()

    @pl.loop(0, tiles)
    def _(tile):
        for kv in range(2):
            write(tile, kv).wait()


def interleave(first, row_len, new, own, pieces, caches):
    count, dim = pieces[0].shape[1:]
    block = BLOCK if count % BLOCK == 0 else BLOCK // 2
    tiles = count // block
    cache = jax.ShapeDtypeStruct((WINDOW * PEERS, dim), jnp.bfloat16)
    any_spec = pl.BlockSpec(memory_space=pltpu.HBM)
    args = [row_len, new, *own, *pieces]
    in_specs = [pl.BlockSpec(memory_space=pltpu.SMEM)] + [pl.BlockSpec(memory_space=pltpu.VMEM)] + [any_spec] * (len(own) + len(pieces))
    aliases = {}
    if caches is not None:
        aliases = {len(args): 0, len(args) + 1: 1}
        args += caches
        in_specs += [any_spec] * 2
    return pl.pallas_call(
        functools.partial(interleave_kernel, first, count, block, len(aliases)),
        out_shape=[cache, cache],
        in_specs=in_specs,
        out_specs=[any_spec] * 2,
        input_output_aliases=aliases,
        scratch_shapes=[
            pltpu.VMEM((tiles, 2, PEERS, block, dim), jnp.bfloat16),
            pltpu.VMEM((tiles, 2, block * PEERS, dim), jnp.bfloat16),
            pltpu.SemaphoreType.DMA((tiles, 2, PEERS)),
            pltpu.SemaphoreType.DMA((tiles, 2)),
        ],
        compiler_params=pltpu.CompilerParams(vmem_limit_bytes=VMEM_LIMIT),
        cost_estimate=pl.CostEstimate(flops=count * 64 * dim, bytes_accessed=count * PEERS * dim * 8, transcendentals=0),
    )(*args)


def small_kernel(first, count, new_ref, *refs):
    pieces = refs[:PEERS]
    k_out, v_out, mixed, sems = refs[PEERS + 2:]
    me = lax.axis_index('sh')
    row_len = jnp.concatenate([new_ref[2].astype(jnp.int32)] * GROUP, axis=0)
    new_slot = row_len & (WINDOW - 1)
    by_offset = pieces[-1:] + tuple(pieces[ORDER.index(offset)] for offset in range(1, PEERS))
    copies = []
    for kv, out in enumerate((k_out, v_out)):
        new = jnp.concatenate([new_ref[kv]] * GROUP, axis=0)
        slot_of_row = lax.broadcasted_iota(jnp.int32, new.shape, 0) // PEERS
        for at in range(0, count, GROUP):
            heads = [ref[kv, at:at + GROUP, :] for ref in by_offset]
            for bit in (1, 2, 4):
                swapped = (me & bit) != 0
                heads = [jnp.where(swapped, heads[head ^ bit], heads[head]) for head in range(PEERS)]
            rows = jnp.swapaxes(jnp.stack(heads, axis=0), 0, 1).reshape(GROUP * PEERS, -1)
            slots = slot_of_row + (first + at)
            rows = jnp.where(slots < row_len, rows.astype(jnp.float32), 0.0)
            rows = jnp.where(slots == new_slot, new, rows)
            mixed[kv, at * PEERS:(at + GROUP) * PEERS, :] = rows.astype(jnp.bfloat16)
        copies.append(pltpu.make_async_copy(mixed.at[kv], out.at[pl.ds(first * PEERS, count * PEERS)], sems.at[kv]))
        copies[-1].start()
    for copy in copies:
        copy.wait()


def interleave_small(first, new, pieces, caches):
    count, dim = pieces[0].shape[1:]
    cache = jax.ShapeDtypeStruct((WINDOW * PEERS, dim), jnp.bfloat16)
    return pl.pallas_call(
        functools.partial(small_kernel, first, count),
        out_shape=[cache, cache],
        in_specs=[pl.BlockSpec(memory_space=pltpu.VMEM)] * (1 + PEERS) + [pl.BlockSpec(memory_space=pltpu.HBM)] * 2,
        out_specs=[pl.BlockSpec(memory_space=pltpu.HBM)] * 2,
        input_output_aliases={1 + PEERS: 0, 2 + PEERS: 1},
        scratch_shapes=[pltpu.VMEM((2, count * PEERS, dim), jnp.bfloat16), pltpu.SemaphoreType.DMA((2,))],
        compiler_params=pltpu.CompilerParams(vmem_limit_bytes=SMALL_VMEM_LIMIT),
        cost_estimate=pl.CostEstimate(flops=count * 64 * dim, bytes_accessed=count * PEERS * dim * 8, transcendentals=0),
    )(new, *pieces, *caches)


def solution(mesh):
    head_spec = P('dp', None, 'sh', None)
    row_spec = P(('dp', 'sh'))
    full_spec = P(None, None)

    def swap(value, offset):
        return lax.ppermute(value, 'sh', [(i, i ^ offset) for i in range(PEERS)])

    def exchange(table, me):
        got = [lax.dynamic_slice_in_dim(table, me ^ offset, 1) for offset in range(PEERS)]
        return [got[0]] + [swap(got[offset], offset) for offset in range(1, PEERS)]

    def by_device(got, me):
        return jnp.take(jnp.concatenate(got, axis=0), me ^ jnp.arange(PEERS), axis=0)

    def per_device(k_prefill, v_prefill, lengths, residual, norm_gain, w_query, w_key, w_value, w_out):
        me = lax.axis_index('sh')
        seq_len = k_prefill.shape[1]
        head_dim = k_prefill.shape[3]
        k_mine = k_prefill.reshape(PEERS, seq_len, head_dim)
        v_mine = v_prefill.reshape(PEERS, seq_len, head_dim)
        my_len = lax.dynamic_slice_in_dim(lengths, me, 1)
        received = {}

        def send(first, pieces, offsets=ORDER):
            received[first] = received.get(first, []) + [swap(piece, offset) for piece, offset in zip(pieces, offsets)]

        def start(chunk, after=None, before=None, offsets=ORDER):
            prefills = (k_mine, v_mine)
            if after is not None:
                prefills, after = lax.optimization_barrier((prefills, after))
            own = (0,) * (chunk[1] <= SMALL and chunk != CHUNKS[0])
            pieces = pack(*chunk, offsets + own, *prefills)
            pieces, before = lax.optimization_barrier((pieces, before))
            send(chunk[0], pieces, offsets)
            received[chunk[0]] += pieces[len(offsets):]
            return after, before

        _, residual = start(CHUNKS[0], before=residual, offsets=ORDER[:1])
        _, residual = start(CHUNKS[0], after=residual, before=residual, offsets=ORDER[1:])
        _, residual = start(CHUNKS[1], after=residual, before=residual)

        resid_f32 = residual.astype(jnp.float32)
        inv_rms = lax.rsqrt(jnp.mean(resid_f32 * resid_f32, axis=-1, keepdims=True) + EPS)
        normed = (resid_f32 * inv_rms * norm_gain.astype(jnp.float32)).astype(jnp.bfloat16)
        q_heads = jnp.dot(normed, w_query, preferred_element_type=jnp.float32).astype(jnp.bfloat16).reshape(1, -1, head_dim)
        k_new = jnp.dot(normed, w_key, preferred_element_type=jnp.float32).astype(jnp.bfloat16).reshape(1, PEERS, head_dim)
        v_new = jnp.dot(normed, w_value, preferred_element_type=jnp.float32).astype(jnp.bfloat16).reshape(1, PEERS, head_dim)
        q_heads = rotate(q_heads, my_len)
        k_new = rotate(k_new, my_len)
        q_group = q_heads.shape[1] // PEERS
        new = jnp.concatenate([k_new.astype(jnp.float32), v_new.astype(jnp.float32), jnp.broadcast_to(my_len.astype(jnp.float32), (1, PEERS, head_dim))], axis=0)

        table = jnp.concatenate([q_heads.reshape(PEERS, q_group, head_dim), k_new.reshape(PEERS, 1, head_dim), v_new.reshape(PEERS, 1, head_dim)], axis=1).reshape(PEERS, -1)
        qkv_parts = exchange(table, me)
        _, table = start(CHUNKS[2], after=table, before=table)
        wrap_lengths, _ = lax.optimization_barrier((lengths, table))
        wrapped = wrap_pack(wrap_lengths, k_mine, v_mine)
        send(0, wrapped[:-1])
        received[0] += wrapped[-1:]
        qkv = by_device(qkv_parts, me).reshape(PEERS, q_group + 2, head_dim)
        q_all, k_all, v_all = qkv[:, :q_group], qkv[:, q_group:q_group + 1], qkv[:, q_group + 1:]
        positions = jnp.arange(seq_len, dtype=jnp.int32)[None, :]
        live = (positions < lengths[:, None]) & (positions > lengths[:, None] - WINDOW)
        scores = jnp.einsum('bgd,bsd->bgs', q_all, k_mine, preferred_element_type=jnp.float32) / head_dim ** 0.5
        scores = jnp.where(live[:, None, :], scores, -jnp.inf)
        top_old = jnp.max(scores, axis=-1, keepdims=True)
        new_score = jnp.sum(q_all.astype(jnp.float32) * k_all.astype(jnp.float32), axis=-1, keepdims=True) / head_dim ** 0.5
        top = jnp.maximum(top_old, new_score)
        exp_scores = jnp.exp(scores - top)
        exp_new = jnp.exp(new_score - top)
        total = jnp.sum(exp_scores, axis=-1, keepdims=True) + exp_new
        weights = (exp_scores / total).astype(jnp.bfloat16)
        new_weight = lax.reduce_precision(exp_new / total, 8, 7)
        mixed = jnp.einsum('bgs,bsd->bgd', weights, v_mine, preferred_element_type=jnp.float32)
        mixed = (mixed + new_weight * v_all.astype(jnp.float32)).astype(jnp.bfloat16).reshape(PEERS, -1)
        attn_parts = exchange(mixed, me)

        place_len, _ = lax.optimization_barrier((my_len, mixed))
        caches = None

        def store(first, caches):
            if len(received[first]) == PEERS:
                return interleave_small(first, new, received[first], caches)
            return interleave(first, place_len, new, [k_mine, v_mine], received[first], caches)

        caches = store(CHUNKS[0][0], caches)
        caches = store(CHUNKS[1][0], caches)
        caches, caches = start(CHUNKS[3], after=caches, before=caches)
        caches, caches = start(CHUNKS[4], after=caches, before=caches)
        caches = store(CHUNKS[2][0], caches)
        caches, caches = start(CHUNKS[5], after=caches, before=caches)
        attn_parts, caches = lax.optimization_barrier((attn_parts, caches))
        attn_out = by_device(attn_parts, me).reshape(1, -1)
        resid_out = (resid_f32 + jnp.dot(attn_out, w_out, preferred_element_type=jnp.float32)).astype(jnp.bfloat16)
        for first in (0,) + tuple(chunk[0] for chunk in CHUNKS[3:]):
            caches = store(first, caches)
        shape = (1, WINDOW, PEERS, head_dim)
        return resid_out, caches[0].reshape(shape), caches[1].reshape(shape)

    return jax.shard_map(per_device, mesh=mesh, in_specs=(head_spec, head_spec, P('dp'), P(('dp', 'sh'), None), P(None), full_spec, full_spec, full_spec, full_spec), out_specs=(P(('dp', 'sh'), None), row_spec, row_spec), check_vma=False)
```

```python
import functools

import jax
import jax.numpy as jnp
from jax import lax
from jax.experimental import pallas as pl
from jax.experimental.pallas import tpu as pltpu
from jax.sharding import PartitionSpec as P


WINDOW = 4096
THETA = 10000.0
EPS = 1e-5
PEERS = 8
GROUP = 32
WRAP = 256
SMALL = 256
CHUNKS = ((256, 512), (768, 1024), (1792, 1280), (3072, 640), (3712, 256), (3968, 128))
BLOCK = 256
ORDER = (6, 4, 2, 7, 5, 3, 1)
VMEM_LIMIT = 56 * 1024 * 1024
SMALL_VMEM_LIMIT = 8 * 1024 * 1024


def rotate(heads, positions):
    head_dim = heads.shape[-1]
    half_dim = head_dim // 2
    inv_freq = THETA ** (-2.0 * jnp.arange(half_dim, dtype=jnp.float32) / head_dim)
    angles = positions.astype(jnp.float32).reshape(positions.shape + (1,) * (heads.ndim - 1)) * inv_freq
    cos_part = jnp.cos(angles)
    sin_part = jnp.sin(angles)
    first_half = heads[..., :half_dim].astype(jnp.float32)
    second_half = heads[..., half_dim:].astype(jnp.float32)
    return jnp.concatenate([first_half * cos_part - second_half * sin_part, second_half * cos_part + first_half * sin_part], axis=-1).astype(jnp.bfloat16)


def pack_kernel(first, count, offsets, k_ref, v_ref, *refs):
    outs, sems = refs[:-1], refs[-1]
    me = lax.axis_index('sh')
    copies = []
    for at, offset in enumerate(offsets):
        for kv, src in enumerate((k_ref, v_ref)):
            copies.append(pltpu.make_async_copy(src.at[me ^ offset, pl.ds(first, count)], outs[at].at[kv], sems.at[at, kv]))
            copies[-1].start()
    for copy in copies:
        copy.wait()


def pack(first, count, offsets, k_mine, v_mine):
    dim = k_mine.shape[2]
    pieces = len(offsets)
    piece = pltpu.VMEM if first == CHUNKS[0][0] or count <= SMALL else jax.ShapeDtypeStruct
    return pl.pallas_call(
        functools.partial(pack_kernel, first, count, offsets),
        out_shape=[piece((2, count, dim), jnp.bfloat16)] * pieces,
        in_specs=[pl.BlockSpec(memory_space=pltpu.HBM)] * 2,
        out_specs=[pl.BlockSpec(memory_space=pltpu.VMEM)] * pieces,
        scratch_shapes=[pltpu.SemaphoreType.DMA((pieces, 2))],
        compiler_params=pltpu.CompilerParams(vmem_limit_bytes=VMEM_LIMIT),
        cost_estimate=pl.CostEstimate(flops=0, bytes_accessed=pieces * 4 * count * dim * 2, transcendentals=0),
    )(k_mine, v_mine)


def wrap_kernel(len_ref, k_ref, k_late_ref, v_ref, v_late_ref, *outs):
    me = lax.axis_index('sh')
    slots = lax.broadcasted_iota(jnp.int32, (WRAP, 128), 0)
    for out, offset in zip(outs, ORDER + (0,)):
        row = me ^ offset
        late = slots + WINDOW < len_ref[row]
        for kv, (base_ref, late_ref) in enumerate(((k_ref, k_late_ref), (v_ref, v_late_ref))):
            out[kv] = jnp.where(late, late_ref[row].astype(jnp.float32), base_ref[row].astype(jnp.float32)).astype(jnp.bfloat16)


def wrap_pack(lengths, k_mine, v_mine):
    rows, _, dim = k_mine.shape
    base = pl.BlockSpec((rows, WRAP, dim), lambda i: (0, 0, 0))
    late = pl.BlockSpec((rows, WRAP, dim), lambda i: (0, WINDOW // WRAP, 0))
    piece = jax.ShapeDtypeStruct((2, WRAP, dim), jnp.bfloat16)
    return pl.pallas_call(
        wrap_kernel,
        grid=(1,),
        out_shape=[piece] * (len(ORDER) + 1),
        out_specs=[pl.BlockSpec((2, WRAP, dim), lambda i: (0, 0, 0))] * (len(ORDER) + 1),
        in_specs=[pl.BlockSpec(memory_space=pltpu.SMEM), base, late, base, late],
        compiler_params=pltpu.CompilerParams(vmem_limit_bytes=VMEM_LIMIT),
        cost_estimate=pl.CostEstimate(flops=rows * 8 * WRAP * dim, bytes_accessed=rows * 6 * WRAP * dim * 2, transcendentals=0),
    )(lengths, k_mine, k_mine, v_mine, v_mine)


def interleave_kernel(first, count, block, num_alias, len_ref, new_ref, *refs):
    own = refs[:2]
    pieces = refs[2:2 + len(ORDER)]
    k_out, v_out, held, mixed, in_sems, out_sems = refs[2 + len(ORDER) + num_alias:]
    tiles = count // block
    me = lax.axis_index('sh')
    row_len = len_ref[0]
    new_slot = lax.rem(row_len, WINDOW)
    outs = (k_out, v_out)

    def read(tile, kv, offset):
        at = pl.multiple_of(tile * block, block)
        if offset:
            src = pieces[ORDER.index(offset)].at[kv, pl.ds(at, block)]
        else:
            src = own[kv].at[me, pl.ds(first + at, block)]
        return pltpu.make_async_copy(src, held.at[tile, kv, me ^ offset], in_sems.at[tile, kv, offset])

    def write(tile, kv):
        at = pl.multiple_of((first + tile * block) * PEERS, block * PEERS)
        return pltpu.make_async_copy(mixed.at[tile, kv], outs[kv].at[pl.ds(at, block * PEERS)], out_sems.at[tile, kv])

    @pl.loop(0, tiles)
    def _(tile):
        for kv in range(2):
            for offset in range(PEERS):
                read(tile, kv, offset).start()

    @pl.loop(0, tiles)
    def _(tile):
        start = first + tile * block
        plain = (start + block <= row_len) & ((new_slot < start) | (new_slot >= start + block))
        for kv in range(2):
            for offset in range(PEERS):
                read(tile, kv, offset).wait()

            def group(at):
                return jnp.swapaxes(held[tile, kv, :, at:at + GROUP, :], 0, 1).reshape(GROUP * PEERS, -1)

            @pl.when(plain)
            def _():
                for at in range(0, block, GROUP):
                    mixed[tile, kv, at * PEERS:(at + GROUP) * PEERS, :] = group(at)

            @pl.when(jnp.logical_not(plain))
            def _():
                new = jnp.concatenate([new_ref[kv]] * GROUP, axis=0)
                slot_of_row = lax.broadcasted_iota(jnp.int32, new.shape, 0) // PEERS
                for at in range(0, block, GROUP):
                    slots = slot_of_row + (start + at)
                    rows = jnp.where(slots < row_len, group(at).astype(jnp.float32), 0.0)
                    rows = jnp.where(slots == new_slot, new, rows)
                    mixed[tile, kv, at * PEERS:(at + GROUP) * PEERS, :] = rows.astype(jnp.bfloat16)

            write(tile, kv).start()

    @pl.loop(0, tiles)
    def _(tile):
        for kv in range(2):
            write(tile, kv).wait()


def interleave(first, row_len, new, own, pieces, caches):
    count, dim = pieces[0].shape[1:]
    block = BLOCK if count % BLOCK == 0 else BLOCK // 2
    tiles = count // block
    cache = jax.ShapeDtypeStruct((WINDOW * PEERS, dim), jnp.bfloat16)
    any_spec = pl.BlockSpec(memory_space=pltpu.HBM)
    args = [row_len, new, *own, *pieces]
    in_specs = [pl.BlockSpec(memory_space=pltpu.SMEM)] + [pl.BlockSpec(memory_space=pltpu.VMEM)] + [any_spec] * (len(own) + len(pieces))
    aliases = {}
    if caches is not None:
        aliases = {len(args): 0, len(args) + 1: 1}
        args += caches
        in_specs += [any_spec] * 2
    return pl.pallas_call(
        functools.partial(interleave_kernel, first, count, block, len(aliases)),
        out_shape=[cache, cache],
        in_specs=in_specs,
        out_specs=[any_spec] * 2,
        input_output_aliases=aliases,
        scratch_shapes=[
            pltpu.VMEM((tiles, 2, PEERS, block, dim), jnp.bfloat16),
            pltpu.VMEM((tiles, 2, block * PEERS, dim), jnp.bfloat16),
            pltpu.SemaphoreType.DMA((tiles, 2, PEERS)),
            pltpu.SemaphoreType.DMA((tiles, 2)),
        ],
        compiler_params=pltpu.CompilerParams(vmem_limit_bytes=VMEM_LIMIT),
        cost_estimate=pl.CostEstimate(flops=count * 64 * dim, bytes_accessed=count * PEERS * dim * 8, transcendentals=0),
    )(*args)


def small_kernel(first, count, new_ref, *refs):
    pieces = refs[:PEERS]
    k_out, v_out, mixed, sems = refs[PEERS + 2:]
    me = lax.axis_index('sh')
    row_len = jnp.concatenate([new_ref[2].astype(jnp.int32)] * GROUP, axis=0)
    new_slot = row_len & (WINDOW - 1)
    by_offset = pieces[-1:] + tuple(pieces[ORDER.index(offset)] for offset in range(1, PEERS))
    copies = []
    for kv, out in enumerate((k_out, v_out)):
        new = jnp.concatenate([new_ref[kv]] * GROUP, axis=0)
        slot_of_row = lax.broadcasted_iota(jnp.int32, new.shape, 0) // PEERS
        for at in range(0, count, GROUP):
            heads = [ref[kv, at:at + GROUP, :] for ref in by_offset]
            for bit in (1, 2, 4):
                swapped = (me & bit) != 0
                heads = [jnp.where(swapped, heads[head ^ bit], heads[head]) for head in range(PEERS)]
            rows = jnp.swapaxes(jnp.stack(heads, axis=0), 0, 1).reshape(GROUP * PEERS, -1)
            slots = slot_of_row + (first + at)
            rows = jnp.where(slots < row_len, rows.astype(jnp.float32), 0.0)
            rows = jnp.where(slots == new_slot, new, rows)
            mixed[kv, at * PEERS:(at + GROUP) * PEERS, :] = rows.astype(jnp.bfloat16)
        copies.append(pltpu.make_async_copy(mixed.at[kv], out.at[pl.ds(first * PEERS, count * PEERS)], sems.at[kv]))
        copies[-1].start()
    for copy in copies:
        copy.wait()


def interleave_small(first, new, pieces, caches):
    count, dim = pieces[0].shape[1:]
    cache = jax.ShapeDtypeStruct((WINDOW * PEERS, dim), jnp.bfloat16)
    return pl.pallas_call(
        functools.partial(small_kernel, first, count),
        out_shape=[cache, cache],
        in_specs=[pl.BlockSpec(memory_space=pltpu.VMEM)] * (1 + PEERS) + [pl.BlockSpec(memory_space=pltpu.HBM)] * 2,
        out_specs=[pl.BlockSpec(memory_space=pltpu.HBM)] * 2,
        input_output_aliases={1 + PEERS: 0, 2 + PEERS: 1},
        scratch_shapes=[pltpu.VMEM((2, count * PEERS, dim), jnp.bfloat16), pltpu.SemaphoreType.DMA((2,))],
        compiler_params=pltpu.CompilerParams(vmem_limit_bytes=SMALL_VMEM_LIMIT),
        cost_estimate=pl.CostEstimate(flops=count * 64 * dim, bytes_accessed=count * PEERS * dim * 8, transcendentals=0),
    )(new, *pieces, *caches)


def solution(mesh):
    head_spec = P('dp', None, 'sh', None)
    row_spec = P(('dp', 'sh'))
    full_spec = P(None, None)

    def swap(value, offset):
        return lax.ppermute(value, 'sh', [(i, i ^ offset) for i in range(PEERS)])

    def exchange(table, me):
        got = [lax.dynamic_slice_in_dim(table, me ^ offset, 1) for offset in range(PEERS)]
        return [got[0]] + [swap(got[offset], offset) for offset in range(1, PEERS)]

    def by_device(got, me):
        return jnp.take(jnp.concatenate(got, axis=0), me ^ jnp.arange(PEERS), axis=0)

    def per_device(k_prefill, v_prefill, lengths, residual, norm_gain, w_query, w_key, w_value, w_out):
        me = lax.axis_index('sh')
        seq_len = k_prefill.shape[1]
        head_dim = k_prefill.shape[3]
        k_mine = k_prefill.reshape(PEERS, seq_len, head_dim)
        v_mine = v_prefill.reshape(PEERS, seq_len, head_dim)
        my_len = lax.dynamic_slice_in_dim(lengths, me, 1)
        received = {}

        def send(first, pieces, offsets=ORDER):
            received[first] = received.get(first, []) + [swap(piece, offset) for piece, offset in zip(pieces, offsets)]

        def start(chunk, after=None, before=None, offsets=ORDER):
            prefills = (k_mine, v_mine)
            if after is not None:
                prefills, after = lax.optimization_barrier((prefills, after))
            own = (0,) * (chunk[1] <= SMALL and chunk != CHUNKS[0])
            pieces = pack(*chunk, offsets + own, *prefills)
            pieces, before = lax.optimization_barrier((pieces, before))
            send(chunk[0], pieces, offsets)
            received[chunk[0]] += pieces[len(offsets):]
            return after, before

        _, residual = start(CHUNKS[0], before=residual, offsets=ORDER[:1])
        _, residual = start(CHUNKS[0], after=residual, before=residual, offsets=ORDER[1:])
        _, residual = start(CHUNKS[1], after=residual, before=residual)

        resid_f32 = residual.astype(jnp.float32)
        inv_rms = lax.rsqrt(jnp.mean(resid_f32 * resid_f32, axis=-1, keepdims=True) + EPS)
        normed = (resid_f32 * inv_rms * norm_gain.astype(jnp.float32)).astype(jnp.bfloat16)
        q_heads = jnp.dot(normed, w_query, preferred_element_type=jnp.float32).astype(jnp.bfloat16).reshape(1, -1, head_dim)
        k_new = jnp.dot(normed, w_key, preferred_element_type=jnp.float32).astype(jnp.bfloat16).reshape(1, PEERS, head_dim)
        v_new = jnp.dot(normed, w_value, preferred_element_type=jnp.float32).astype(jnp.bfloat16).reshape(1, PEERS, head_dim)
        q_heads = rotate(q_heads, my_len)
        k_new = rotate(k_new, my_len)
        q_group = q_heads.shape[1] // PEERS
        new = jnp.concatenate([k_new.astype(jnp.float32), v_new.astype(jnp.float32), jnp.broadcast_to(my_len.astype(jnp.float32), (1, PEERS, head_dim))], axis=0)

        table = jnp.concatenate([q_heads.reshape(PEERS, q_group, head_dim), k_new.reshape(PEERS, 1, head_dim), v_new.reshape(PEERS, 1, head_dim)], axis=1).reshape(PEERS, -1)
        qkv_parts = exchange(table, me)
        _, table = start(CHUNKS[2], after=table, before=table)
        wrap_lengths, _ = lax.optimization_barrier((lengths, table))
        wrapped = wrap_pack(wrap_lengths, k_mine, v_mine)
        send(0, wrapped[:-1])
        received[0] += wrapped[-1:]
        qkv = by_device(qkv_parts, me).reshape(PEERS, q_group + 2, head_dim)
        q_all, k_all, v_all = qkv[:, :q_group], qkv[:, q_group:q_group + 1], qkv[:, q_group + 1:]
        positions = jnp.arange(seq_len, dtype=jnp.int32)[None, :]
        live = (positions < lengths[:, None]) & (positions > lengths[:, None] - WINDOW)
        scores = jnp.einsum('bgd,bsd->bgs', q_all, k_mine, preferred_element_type=jnp.float32) / head_dim ** 0.5
        scores = jnp.where(live[:, None, :], scores, -jnp.inf)
        top_old = jnp.max(scores, axis=-1, keepdims=True)
        new_score = jnp.sum(q_all.astype(jnp.float32) * k_all.astype(jnp.float32), axis=-1, keepdims=True) / head_dim ** 0.5
        top = jnp.maximum(top_old, new_score)
        exp_scores = jnp.exp(scores - top)
        exp_new = jnp.exp(new_score - top)
        total = jnp.sum(exp_scores, axis=-1, keepdims=True) + exp_new
        weights = (exp_scores / total).astype(jnp.bfloat16)
        new_weight = lax.reduce_precision(exp_new / total, 8, 7)
        mixed = jnp.einsum('bgs,bsd->bgd', weights, v_mine, preferred_element_type=jnp.float32)
        mixed = (mixed + new_weight * v_all.astype(jnp.float32)).astype(jnp.bfloat16).reshape(PEERS, -1)
        attn_parts = exchange(mixed, me)

        place_len, _ = lax.optimization_barrier((my_len, mixed))
        caches = None

        def store(first, caches):
            if len(received[first]) == PEERS:
                return interleave_small(first, new, received[first], caches)
            return interleave(first, place_len, new, [k_mine, v_mine], received[first], caches)

        caches = store(CHUNKS[0][0], caches)
        caches = store(CHUNKS[1][0], caches)
        caches, caches = start(CHUNKS[3], after=caches, before=caches)
        caches, caches = start(CHUNKS[4], after=caches, before=caches)
        caches = store(CHUNKS[2][0], caches)
        caches, caches = start(CHUNKS[5], after=caches, before=caches)
        attn_parts, caches = lax.optimization_barrier((attn_parts, caches))
        attn_out = by_device(attn_parts, me).reshape(1, -1)
        resid_out = (resid_f32 + jnp.dot(attn_out, w_out, preferred_element_type=jnp.float32)).astype(jnp.bfloat16)
        for first in (0,) + tuple(chunk[0] for chunk in CHUNKS[3:]):
            caches = store(first, caches)
        shape = (1, WINDOW, PEERS, head_dim)
        return resid_out, caches[0].reshape(shape), caches[1].reshape(shape)

    return jax.shard_map(per_device, mesh=mesh, in_specs=(head_spec, head_spec, P('dp'), P(('dp', 'sh'), None), P(None), full_spec, full_spec, full_spec, full_spec), out_specs=(P(('dp', 'sh'), None), row_spec, row_spec), check_vma=False)
```
